32 devices in a mesh: dp: 1 (over z), cp: 32 (over y, x, core).
Axes of the slice: x: 4, y: 4, z: 1, core: 2. Of those that a mesh axis runs over, the one named last changes fastest.
The devices are a block of a 4x4x8 slice.
Arguments:
- hidden: bfloat16 [8192, 1152], P(('dp', 'cp'))
- w_query: bfloat16 [6, 1152, 4, 256], replicated
- w_key: bfloat16 [6, 1152, 4, 256], replicated
- w_value: bfloat16 [6, 1152, 4, 256], replicated
- w_out: bfloat16 [6, 4, 256, 1152], replicated
Outputs:
- output: bfloat16 [8192, 1152], P(('dp', 'cp'))
All inputs are finite; a program needn't handle non-finite values.
Results may differ from the reference program's by a relative error of at most 0.0126916.
Values are sent between devices in bfloat16 or wider.
A program may use at most 768 MiB of HBM per device.

```python
import jax
import jax.numpy as jnp
from jax import lax

CP_SIZE = 32
TOK_DEV = 256
D_MODEL = 1152
N_HEADS = 4
HEAD_DIM = 256
WINDOW = 1024
LAYERS = 6
SEQ = CP_SIZE * TOK_DEV
N_BACK = min((WINDOW + TOK_DEV - 2) // TOK_DEV, CP_SIZE - 1)
NORM_EPS = 1e-6
NEG_BIG = -1e30


def setup_inputs(seed: int = 0, part: int = 0) -> dict:
    rng_key = jax.random.key(seed)
    part_key = jax.random.fold_in(jax.random.fold_in(rng_key, 1), part)
    keys_w = jax.random.split(jax.random.fold_in(rng_key, 2), 4)
    width = N_HEADS * HEAD_DIM
    out_gain = jnp.where(jnp.arange(LAYERS) == LAYERS - 1, 4.0, 2.0).reshape(LAYERS, 1, 1, 1)
    in_shape = (LAYERS, D_MODEL, N_HEADS, HEAD_DIM)
    hidden = jax.random.normal(part_key, (SEQ, D_MODEL), jnp.float32)
    w_query = jax.random.normal(keys_w[0], in_shape, jnp.float32) * (1.2 * D_MODEL ** -0.5)
    w_key = jax.random.normal(keys_w[1], in_shape, jnp.float32) * D_MODEL ** -0.5
    w_value = jax.random.normal(keys_w[2], in_shape, jnp.float32) * D_MODEL ** -0.5
    w_out = jax.random.normal(keys_w[3], (LAYERS, N_HEADS, HEAD_DIM, D_MODEL), jnp.float32) * out_gain * width ** -0.5
    return {"hidden": hidden.astype(jnp.bfloat16), "w_query": w_query.astype(jnp.bfloat16), "w_key": w_key.astype(jnp.bfloat16), "w_value": w_value.astype(jnp.bfloat16), "w_out": w_out.astype(jnp.bfloat16)}


def rms_norm(hidden):
    hid_f = hidden.astype(jnp.float32)
    return (hid_f * lax.rsqrt(jnp.mean(hid_f * hid_f, axis=-1, keepdims=True) + NORM_EPS)).astype(jnp.bfloat16)


def project(normed, weight):
    flat_w = weight.reshape(D_MODEL, N_HEADS * HEAD_DIM)
    flat_out = jnp.dot(normed, flat_w, preferred_element_type=jnp.float32)
    return flat_out.astype(jnp.bfloat16).reshape(SEQ, N_HEADS, HEAD_DIM)


def empty_state():
    return (jnp.full((TOK_DEV, N_HEADS), NEG_BIG, jnp.float32), jnp.zeros((TOK_DEV, N_HEADS), jnp.float32), jnp.zeros((TOK_DEV, N_HEADS, HEAD_DIM), jnp.float32))


def block_update(soft_state, q_blk, k_blk, v_blk, allowed):
    run_max, run_sum, acc_out = soft_state
    scores = jnp.einsum("qhd,khd->qhk", q_blk.astype(jnp.float32), k_blk.astype(jnp.float32)) * HEAD_DIM ** -0.5
    scores = jnp.where(allowed, scores, NEG_BIG)
    new_max = jnp.maximum(run_max, jnp.max(scores, axis=-1))
    prob_blk = jnp.where(allowed, jnp.exp(scores - new_max[..., None]), 0.0)
    rescale = jnp.exp(run_max - new_max)
    new_sum = run_sum * rescale + jnp.sum(prob_blk, axis=-1)
    prob_low = prob_blk.astype(jnp.bfloat16).astype(jnp.float32)
    new_acc = acc_out * rescale[..., None] + jnp.einsum("qhk,khd->qhd", prob_low, v_blk.astype(jnp.float32))
    return new_max, new_sum, new_acc


def finish(soft_state):
    run_max, run_sum, acc_out = soft_state
    return (acc_out / run_sum[..., None]).astype(jnp.bfloat16)


def local_attention(q_all, k_all, v_all):
    q_blocks = q_all.reshape(CP_SIZE, TOK_DEV, N_HEADS, HEAD_DIM)
    zero_pad = jnp.zeros((N_BACK * TOK_DEV, N_HEADS, HEAD_DIM), k_all.dtype)
    k_blocks = jnp.concatenate([zero_pad, k_all], axis=0).reshape(CP_SIZE + N_BACK, TOK_DEV, N_HEADS, HEAD_DIM)
    v_blocks = jnp.concatenate([zero_pad, v_all], axis=0).reshape(CP_SIZE + N_BACK, TOK_DEV, N_HEADS, HEAD_DIM)
    offsets = jnp.arange(TOK_DEV)

    def one_block(q_args):
        q_blk, blk_idx = q_args
        q_pos = blk_idx * TOK_DEV + offsets
        soft_state = empty_state()
        for back_idx in range(N_BACK + 1):
            k_blk = lax.dynamic_index_in_dim(k_blocks, blk_idx + N_BACK - back_idx, 0, keepdims=False)
            v_blk = lax.dynamic_index_in_dim(v_blocks, blk_idx + N_BACK - back_idx, 0, keepdims=False)
            k_pos = (blk_idx - back_idx) * TOK_DEV + offsets
            pos_gap = q_pos[:, None] - k_pos[None, :]
            allowed = (pos_gap >= 0) & (pos_gap < WINDOW) & (k_pos[None, :] >= 0)
            soft_state = block_update(soft_state, q_blk, k_blk, v_blk, allowed[:, None, :])
        return finish(soft_state)

    attn_out = lax.map(one_block, (q_blocks, jnp.arange(CP_SIZE)))
    return attn_out.reshape(SEQ, N_HEADS, HEAD_DIM)


def global_attention(q_all, k_all, v_all):
    q_blocks = q_all.reshape(CP_SIZE, TOK_DEV, N_HEADS, HEAD_DIM)
    k_blocks = k_all.reshape(CP_SIZE, TOK_DEV, N_HEADS, HEAD_DIM)
    v_blocks = v_all.reshape(CP_SIZE, TOK_DEV, N_HEADS, HEAD_DIM)
    offsets = jnp.arange(TOK_DEV)

    def one_block(q_args):
        q_blk, blk_idx = q_args
        q_pos = blk_idx * TOK_DEV + offsets

        def key_step(soft_state, kv_args):
            k_blk, v_blk, kb_idx = kv_args
            k_pos = kb_idx * TOK_DEV + offsets
            allowed = k_pos[None, :] <= q_pos[:, None]
            return block_update(soft_state, q_blk, k_blk, v_blk, allowed[:, None, :]), None

        soft_state, unused_out = lax.scan(key_step, empty_state(), (k_blocks, v_blocks, jnp.arange(CP_SIZE)))
        return finish(soft_state)

    attn_out = lax.map(one_block, (q_blocks, jnp.arange(CP_SIZE)))
    return attn_out.reshape(SEQ, N_HEADS, HEAD_DIM)


def attn_layer(hidden, w_query, w_key, w_value, w_out, attend):
    normed = rms_norm(hidden)
    attn_out = attend(project(normed, w_query), project(normed, w_key), project(normed, w_value))
    out_proj = jnp.dot(attn_out.reshape(SEQ, N_HEADS * HEAD_DIM), w_out.reshape(N_HEADS * HEAD_DIM, D_MODEL), preferred_element_type=jnp.float32)
    return (hidden.astype(jnp.float32) + out_proj).astype(jnp.bfloat16)


def reference(hidden, w_query, w_key, w_value, w_out):
    def local_step(hid_state, layer_w):
        return attn_layer(hid_state, layer_w[0], layer_w[1], layer_w[2], layer_w[3], local_attention), None

    last = LAYERS - 1
    hidden, unused_out = lax.scan(local_step, hidden, (w_query[:last], w_key[:last], w_value[:last], w_out[:last]))
    return attn_layer(hidden, w_query[last], w_key[last], w_value[last], w_out[last], global_attention)
```

```python
import functools
import math

import jax
import jax.numpy as jnp
from jax import lax
from jax.experimental import pallas as pl
from jax.experimental.pallas import tpu as pltpu
from jax.sharding import PartitionSpec as P

WINDOW = 1024
NORM_EPS = 1e-6
NEG_BIG = -1e30
BF16 = jnp.bfloat16
F32 = jnp.float32
LANES = 128
N_T1 = 160

STAGE_OFF = (None, 0, -1, 1, 2)
EVENTS = (("near", 0), ("near", 1), ("opp", 0), ("near", 2), ("near", 3),
          ("opp", 1), ("near", 4), ("opp", 2), ("opp", 3), ("opp", 4))


def stage_units(kind, stage):
    dists = (-1, 1) if kind == "near" else (2,)
    if stage == 0:
        return [(dist, 0) for dist in dists]
    return [(STAGE_OFF[stage], dist) for dist in dists]


UNITS = []
EVENT_START = []
for ev_kind, ev_stage in EVENTS:
    EVENT_START.append(len(UNITS))
    for half_idx in range(2):
        for off in stage_units(ev_kind, ev_stage):
            UNITS.append((half_idx,) + off)


def flat_view(weight):
    n_layers, d_model, n_heads, head_dim = weight.shape
    split = weight.reshape(n_layers, d_model, n_heads, head_dim // LANES, LANES)
    return split.transpose(0, 1, 3, 2, 4).reshape(n_layers, -1, LANES)


def table(index, values):
    out = jnp.int32(values[0])
    for pos, value in enumerate(values):
        if pos and value != values[0]:
            out = jnp.where(index == pos, jnp.int32(value), out)
    return out


def kernel(n_cp, n_layers, n_heads, head_dim, x_in, wq, wk, wv, wo, out,
           xb, hown, h1, h2, relay, hfull, raw, fs, wc, wob, qb, kb, vb,
           acc, m_st, l_st, obuf, osend,
           raw_sem, wo_sem, ls, lr, gs, gr, ds, dr):
    n_tok, d_model = x_in.shape
    n_chip = n_cp // 2
    side = math.isqrt(n_chip)
    half_w = n_heads // 2 * head_dim
    n_ct = head_dim // LANES
    n_t2 = n_tok - N_T1
    quarter = n_tok // 2
    eighth = quarter // 2
    scale = head_dim ** -0.5
    me = lax.axis_index("cp")
    chip = me // 2
    core = me % 2
    other = 1 - core
    px, py = chip % side, chip // side

    def at_xy(x, y):
        return ((y + side) % side) * side + (x + side) % side

    def ring(step):
        return (chip + n_chip + step) % n_chip

    def dev(c, k=None):
        return {"cp": c * 2 + (core if k is None else k)}

    nxt, prv = ring(1), ring(-1)
    xm, xp = at_xy(px - 1, py), at_xy(px + 1, py)
    ym, yp = at_xy(px, py - 1), at_xy(px, py + 1)
    skip_to = (xp + 2) % n_chip
    back2 = ring(-2)
    skip_from = at_xy(back2 % side - 1, back2 // side)

    barrier = pltpu.get_barrier_semaphore()
    peers = [dev(c) for c in (nxt, prv, xm, xp, ym, yp, skip_to, skip_from)] + [dev(chip, other)]
    for peer in peers:
        pl.semaphore_signal(barrier, inc=1, device_id=peer, device_id_type=pl.DeviceIdType.MESH)

    def raw_copies(layer):
        return [pltpu.make_async_copy(w.at[layer], raw.at[i], raw_sem.at[i]) for i, w in enumerate((wq, wk, wv))]

    def wo_copy(layer):
        slot = layer % 2
        return pltpu.make_async_copy(wo.at[layer], wob.at[slot], wo_sem.at[slot])

    for cp in raw_copies(0):
        cp.start()
    wo_copy(0).start()
    xb[...] = x_in[...]
    pl.semaphore_wait(barrier, len(peers))

    def convert(layer):
        slot = layer % 2
        d_step = fs.shape[0] // (n_heads * n_ct)
        for cp in raw_copies(layer):
            cp.wait()
        for i in range(3):
            def chunk(j, carry):
                r0 = pl.multiple_of(j * fs.shape[0], fs.shape[0])
                d0 = pl.multiple_of(j * d_step, d_step)
                fs[...] = raw[i, pl.ds(r0, fs.shape[0]), :].astype(F32)
                for hd in range(n_heads // 2):
                    for ct in range(n_ct):
                        first = ct * n_heads + core * (n_heads // 2) + hd
                        piece = fs[pl.ds(first, d_step, stride=n_heads * n_ct), :]
                        wc[slot, i, pl.ds(d0, d_step), pl.ds(hd * head_dim + ct * LANES, LANES)] = piece.astype(BF16)
                return carry
            lax.fori_loop(0, d_model // d_step, chunk, 0)

    def project(rows, slot, which, dst, factor=None):
        for j in range(half_w // head_dim):
            cols = pl.ds(j * head_dim, head_dim)
            val = jnp.dot(rows, wc[slot, which, :, cols], preferred_element_type=F32).astype(BF16)
            if factor is not None:
                val = val * BF16(factor)
            dst[:, cols] = val

    def update(qi, hd, k_ref, v_ref, mask=None, first=False):
        idx = qi * (n_heads // 2) + hd
        cols = pl.ds(hd * head_dim, head_dim)
        s = lax.dot_general(qb[qi, :, cols], k_ref[:, cols], (((1,), (1,)), ((), ())), preferred_element_type=F32)
        if mask is not None:
            s = jnp.where(mask, s, NEG_BIG)
        top = jnp.max(s, axis=1, keepdims=True)
        if first:
            new_m = top
        else:
            old_m = m_st[idx, :, :1]
            new_m = jnp.maximum(old_m, top)
        p = jnp.exp(s - new_m)
        row_sum = jnp.sum(p, axis=1, keepdims=True)
        pv = jnp.dot(p.astype(BF16), v_ref[:, cols], preferred_element_type=F32)
        if first:
            l_st[idx] = jnp.broadcast_to(row_sum, l_st.shape[1:])
            acc[idx] = pv
        else:
            alpha = jnp.exp(old_m - new_m)
            l_st[idx] = jnp.broadcast_to(l_st[idx, :, :1] * alpha + row_sum, l_st.shape[1:])
            acc[idx] = acc[idx] * alpha + pv
        m_st[idx] = jnp.broadcast_to(new_m, m_st.shape[1:])

    def normed():
        xf = xb[...].astype(F32)
        return (xf * lax.rsqrt(jnp.mean(xf * xf, axis=-1, keepdims=True) + NORM_EPS)).astype(BF16)

    def o_copy(layer):
        return pltpu.make_async_remote_copy(osend, obuf.at[core], ls.at[layer, 10], lr.at[layer, 10],
                                            device_id=dev(chip, other), device_id_type=pl.DeviceIdType.MESH)

    def out_update(layer):
        slot = layer % 2
        for j in range(d_model // 384):
            cols = pl.ds(j * 384, 384)
            tot = xb[:, cols].astype(F32)
            prod = jnp.dot(obuf[0], wob[slot, :half_w, cols], preferred_element_type=F32)
            prod = prod + jnp.dot(obuf[1], wob[slot, half_w:, cols], preferred_element_type=F32)
            xb[:, cols] = (tot + prod).astype(BF16)

    def ici(layer, i, src, dst, c, k=None):
        return pltpu.make_async_remote_copy(src, dst, ls.at[layer, i], lr.at[layer, i],
                                            device_id=dev(c, k), device_id_type=pl.DeviceIdType.MESH)

    row_i = lax.broadcasted_iota(jnp.int32, (n_tok, n_tok), 0)
    col_i = lax.broadcasted_iota(jnp.int32, (n_tok, n_tok), 1)

    def local_layer(layer, carry):
        slot = layer % 2
        mine = pl.ds(pl.multiple_of(core * n_tok, n_tok), n_tok)
        theirs = pl.ds(pl.multiple_of(other * n_tok, n_tok), n_tok)
        k1 = pl.ds(pl.multiple_of(core * N_T1, 16), N_T1)
        k2 = pl.ds(pl.multiple_of(core * n_t2, 16), n_t2)
        o1 = pl.ds(pl.multiple_of(other * N_T1, 16), N_T1)
        o2 = pl.ds(pl.multiple_of(other * n_t2, 16), n_t2)
        hown[mine, :] = normed()
        own1 = hown.at[pl.ds(pl.multiple_of(core * n_tok, n_tok), N_T1), :]
        own2 = hown.at[pl.ds(pl.multiple_of(core * n_tok + N_T1, 16), n_t2), :]
        near1, far1 = h1.at[layer, 0], h1.at[layer, 1]
        near2, far2 = h2.at[layer, 0], h2.at[layer, 1]
        rl = relay.at[layer]
        t1_own = ici(layer, 0, own1, near1.at[k1], nxt)
        t2_own = ici(layer, 1, own2, rl, xm)
        d_own = ici(layer, 2, hown.at[mine], hown.at[mine], chip, other)
        t2_relay = ici(layer, 3, rl, far2.at[k2], skip_to)
        t1_fwd = ici(layer, 4, near1.at[k1], far1.at[k1], nxt)
        t2_fwd = ici(layer, 5, far2.at[k2], near2.at[k2], prv)
        d_n1 = ici(layer, 6, near1.at[k1], near1.at[k1], chip, other)
        d_f2 = ici(layer, 7, far2.at[k2], far2.at[k2], chip, other)
        d_f1 = ici(layer, 8, far1.at[k1], far1.at[k1], chip, other)
        d_n2 = ici(layer, 9, near2.at[k2], near2.at[k2], chip, other)
        t1_own.start()
        t2_own.start()
        d_own.start()
        wo_copy(layer + 1).start()

        @pl.when(layer == 0)
        def _():
            convert(0)
            for cp in raw_copies(1):
                cp.start()

        def own_block(b, c2):
            rows = hown[pl.ds(pl.multiple_of(b * n_tok, n_tok), n_tok), :]
            dst_rows = pl.ds(pl.multiple_of(b * n_tok, n_tok), n_tok)
            project(rows, slot, 0, qb.at[b], scale)
            project(rows, slot, 1, kb.at[0, dst_rows])
            project(rows, slot, 2, vb.at[0, dst_rows])
            return c2

        own_block(core, 0)
        d_own.wait_recv()
        own_block(other, 0)
        causal = col_i <= row_i
        for hd in range(n_heads // 2):
            update(0, hd, kb.at[0, :n_tok], vb.at[0, :n_tok], causal, first=True)
            update(1, hd, kb.at[0, n_tok:], vb.at[0, n_tok:], causal, first=True)
            update(1, hd, kb.at[0, :n_tok], vb.at[0, :n_tok])
        convert(layer + 1)

        @pl.when(layer + 2 < n_layers)
        def _():
            for cp in raw_copies(layer + 2):
                cp.start()

        t2_own.wait_recv()
        t2_relay.start()
        t1_own.wait_recv()
        t1_fwd.start()
        d_n1.start()

        def kv_rows(rows, which, lo, n):
            project(rows, slot, 1, kb.at[which, pl.ds(lo, n)])
            project(rows, slot, 2, vb.at[which, pl.ds(lo, n)])

        d_n1.wait_recv()

        @pl.when(chip >= 1)
        def _():
            kv_rows(near1[...], 1, 0, 2 * N_T1)
        t2_relay.wait_recv()
        t2_fwd.start()
        d_f2.start()
        d_f2.wait_recv()

        @pl.when(chip >= 2)
        def _():
            kv_rows(far2[...], 2, 2 * N_T1, 2 * n_t2)
        t1_fwd.wait_recv()
        d_f1.start()
        t2_fwd.wait_recv()
        d_n2.start()
        d_f1.wait_recv()

        @pl.when(chip >= 2)
        def _():
            kv_rows(far1[...], 2, 0, 2 * N_T1)
            key_j = lax.broadcasted_iota(jnp.int32, (n_tok, 2 * n_tok), 1)
            row_j = lax.broadcasted_iota(jnp.int32, (n_tok, 2 * n_tok), 0)
            in1 = jnp.where(key_j >= N_T1, key_j + n_t2, key_j)
            in2 = jnp.where(key_j >= 2 * N_T1 + n_t2, key_j - N_T1 + N_T1, key_j - N_T1)
            pos = jnp.where(key_j < 2 * N_T1, in1, in2)
            for qi in range(2):
                gap = row_j + qi * n_tok + 4 * n_tok - pos
                for hd in range(n_heads // 2):
                    update(qi, hd, kb.at[2], vb.at[2], gap < WINDOW)
        d_n2.wait_recv()

        @pl.when(chip >= 1)
        def _():
            kv_rows(near2[...], 1, 2 * N_T1, 2 * n_t2)
            for qi in range(2):
                for hd in range(n_heads // 2):
                    update(qi, hd, kb.at[1], vb.at[1])

        def put(qi, dst):
            for hd in range(n_heads // 2):
                idx = qi * (n_heads // 2) + hd
                dst[:, pl.ds(hd * head_dim, head_dim)] = (acc[idx] / l_st[idx, :, :1]).astype(BF16)

        put(other, osend)
        oc = o_copy(layer)
        oc.start()
        put(core, obuf.at[core])
        wo_copy(layer).wait()
        oc.wait_recv()
        out_update(layer)
        for cp in (t1_own, t2_own, d_own, t2_relay, t1_fwd, t2_fwd, d_n1, d_f2, d_f1, d_n2, oc):
            cp.wait_send()
        return carry

    lax.fori_loop(0, n_layers - 1, local_layer, 0)

    last = n_layers - 1
    slot = last % 2
    h_new = normed()
    mine = pl.ds(pl.multiple_of(core * quarter, quarter), quarter)
    for hf in range(2):
        hfull[chip * 2 + hf, mine, :] = h_new[hf * quarter:(hf + 1) * quarter]

    def chip_off(hf, dp, dsec):
        if hf == 0:
            return at_xy(px + dp, py + dsec)
        return at_xy(px + dsec, py + dp)

    def stage_chip(hf, stage, dist):
        if stage == 0:
            return chip_off(hf, dist, 0)
        return chip_off(hf, STAGE_OFF[stage], dist)

    def stage_peer(hf, stage, dist):
        if stage == 0:
            return chip_off(hf, dist, 0)
        return chip_off(hf, 0, dist)

    def g_rows(c, hf, lo, n):
        return hfull.at[c * 2 + hf, pl.ds(pl.multiple_of(core * quarter + lo, 16), n), :]

    def g_copy(hf, stage, kind):
        sgn = 1 if kind % 2 == 0 else -1
        if kind < 2:
            ref = g_rows(stage_chip(hf, stage, 0), hf, 0, quarter)
        else:
            ref = g_rows(stage_chip(hf, stage, -sgn), hf, 0 if kind == 2 else eighth, eighth)
        i = (hf * 5 + stage) * 4 + kind
        return pltpu.make_async_remote_copy(ref, ref, gs.at[i], gr.at[i], device_id=dev(stage_peer(hf, stage, sgn)),
                                            device_id_type=pl.DeviceIdType.MESH)

    def d_copy(i, c, hf):
        ref = g_rows(c, hf, 0, quarter)
        return pltpu.make_async_remote_copy(ref, ref, ds.at[i], dr.at[i], device_id=dev(chip, other),
                                            device_id_type=pl.DeviceIdType.MESH)

    for stage in range(2):
        for hf in range(2):
            for kind in range(2):
                g_copy(hf, stage, kind).start()
    n_units = len(UNITS)
    for hf in range(2):
        d_copy(n_units + hf, chip, hf).start()

    def unit_pos(hf):
        half_row = jnp.where(row_i >= quarter, row_i + quarter, row_i) + hf * quarter
        half_col = jnp.where(col_i >= quarter, col_i + quarter, col_i) + hf * quarter
        return half_row, half_col

    kcat, vcat = kb.at[0], vb.at[0]
    for hf in range(2):
        d_copy(n_units + hf, chip, hf).wait_recv()
        rows = hfull[chip * 2 + hf]
        seg = pl.ds(hf * n_tok, n_tok)
        project(rows, slot, 0, qb.at[hf], scale)
        project(rows, slot, 1, kcat.at[seg])
        project(rows, slot, 2, vcat.at[seg])
    for qi in range(2):
        for ki in range(2):
            mask = unit_pos(ki)[1] <= unit_pos(qi)[0]
            for hd in range(n_heads // 2):
                update(qi, hd, kcat.at[ki * n_tok:(ki + 1) * n_tok], vcat.at[ki * n_tok:(ki + 1) * n_tok], mask, first=ki == 0)

    def run_event(e):
        kind, stage = EVENTS[e]
        at = EVENT_START[e]
        for hf in range(2):
            offs = stage_units(kind, stage)
            if kind == "near":
                for knd in range(2):
                    g_copy(hf, stage, knd).wait_recv()
                for knd in range(2, 4):
                    g_copy(hf, stage, knd).start()
                if stage == 0:
                    for nstage in (2, 3):
                        for knd in range(2):
                            g_copy(hf, nstage, knd).start()
            else:
                for knd in range(2, 4):
                    g_copy(hf, stage, knd).wait_recv()
                if stage == 0:
                    for knd in range(2):
                        g_copy(hf, 4, knd).start()
            for off in offs:
                d_copy(at, chip_off(hf, *off), hf).start()
                at += 1

    def unit_step(i, carry):
        for e in range(len(EVENTS)):
            @pl.when(i == max(0, EVENT_START[e] - 2))
            def _():
                run_event(e)
        hf = table(i, [u[0] for u in UNITS])
        dp = table(i, [u[1] for u in UNITS])
        dsec = table(i, [u[2] for u in UNITS])
        src = at_xy(px + jnp.where(hf == 0, dp, dsec), py + jnp.where(hf == 0, dsec, dp))
        d_copy(i, src, hf).wait_recv()

        @pl.when(src < chip)
        def _():
            rows = hfull[src * 2 + hf]
            k_un, v_un = kb.at[1, :n_tok], vb.at[1, :n_tok]
            project(rows, slot, 1, k_un)
            project(rows, slot, 2, v_un)
            for qi in range(2):
                for hd in range(n_heads // 2):
                    update(qi, hd, k_un, v_un)
        return carry

    lax.fori_loop(0, n_units, unit_step, 0)

    def put_rows(c, dst):
        seg = pl.ds(pl.multiple_of(c * quarter, quarter), quarter)
        for qi in range(2):
            for hd in range(n_heads // 2):
                idx = qi * (n_heads // 2) + hd
                val = acc[idx, seg, :] / l_st[idx, seg, :1]
                dst[qi * quarter:(qi + 1) * quarter, pl.ds(hd * head_dim, head_dim)] = val.astype(BF16)

    put_rows(other, osend)
    oc = o_copy(last)
    oc.start()
    put_rows(core, obuf.at[core])
    wo_copy(last).wait()
    oc.wait_recv()
    out_update(last)
    out[...] = xb[...]
    oc.wait_send()
    for hf in range(2):
        for stage in range(5):
            for kind in range(4):
                g_copy(hf, stage, kind).wait_send()
        d_copy(n_units + hf, chip, hf).wait_send()
    for i in range(n_units):
        hf = UNITS[i][0]
        d_copy(i, chip_off(hf, *UNITS[i][1:]), hf).wait_send()


def solution(mesh):
    n_cp = mesh.shape["cp"]

    def device_body(hidden, w_query, w_key, w_value, w_out):
        n_tok, d_model = hidden.shape
        n_layers, n_heads, head_dim, _ = w_out.shape
        half_w = n_heads // 2 * head_dim
        n_loc = n_layers - 1
        n_t2 = n_tok - N_T1
        flat = n_heads * head_dim // LANES * d_model
        vmem = pl.BlockSpec(memory_space=pltpu.VMEM)
        hbm = pl.BlockSpec(memory_space=pl.ANY)
        scratch = [
            pltpu.VMEM((n_tok, d_model), BF16),
            pltpu.VMEM((2 * n_tok, d_model), BF16),
            pltpu.VMEM((n_loc, 2, 2 * N_T1, d_model), BF16),
            pltpu.VMEM((n_loc, 2, 2 * n_t2, d_model), BF16),
            pltpu.VMEM((n_loc, n_t2, d_model), BF16),
            pltpu.VMEM((n_cp, n_tok, d_model), BF16),
            pltpu.VMEM((3, flat, LANES), BF16),
            pltpu.VMEM((n_heads * head_dim, LANES), F32),
            pltpu.VMEM((2, 3, d_model, half_w), BF16),
            pltpu.VMEM((2, n_heads * head_dim, d_model), BF16),
            pltpu.VMEM((2, n_tok, half_w), BF16),
            pltpu.VMEM((3, 2 * n_tok, half_w), BF16),
            pltpu.VMEM((3, 2 * n_tok, half_w), BF16),
            pltpu.VMEM((n_heads, n_tok, head_dim), F32),
            pltpu.VMEM((n_heads, n_tok, LANES), F32),
            pltpu.VMEM((n_heads, n_tok, LANES), F32),
            pltpu.VMEM((2, n_tok, half_w), BF16),
            pltpu.VMEM((n_tok, half_w), BF16),
            pltpu.SemaphoreType.DMA((3,)),
            pltpu.SemaphoreType.DMA((2,)),
            pltpu.SemaphoreType.DMA((n_layers, 11)),
            pltpu.SemaphoreType.DMA((n_layers, 11)),
            pltpu.SemaphoreType.DMA((40,)),
            pltpu.SemaphoreType.DMA((40,)),
            pltpu.SemaphoreType.DMA((len(UNITS) + 2,)),
            pltpu.SemaphoreType.DMA((len(UNITS) + 2,)),
        ]
        return pl.pallas_call(
            functools.partial(kernel, n_cp, n_layers, n_heads, head_dim),
            out_shape=jax.ShapeDtypeStruct(hidden.shape, hidden.dtype),
            in_specs=[vmem, hbm, hbm, hbm, hbm],
            out_specs=vmem,
            scratch_shapes=scratch,
            compiler_params=pltpu.CompilerParams(collective_id=0, has_side_effects=True, vmem_limit_bytes=66_500_000),
        )(hidden, flat_view(w_query), flat_view(w_key), flat_view(w_value),
          w_out.reshape(n_layers, n_heads * head_dim, d_model))

    row_spec = P(("dp", "cp"), None)
    return jax.shard_map(device_body, mesh=mesh, in_specs=(row_spec, P(), P(), P(), P()), out_specs=row_spec, check_vma=False)
```

```python
import functools
import math

import jax
import jax.numpy as jnp
from jax import lax
from jax.experimental import pallas as pl
from jax.experimental.pallas import tpu as pltpu
from jax.sharding import PartitionSpec as P

WINDOW = 1024
NORM_EPS = 1e-6
NEG_BIG = -1e30
BF16 = jnp.bfloat16
F32 = jnp.float32
LANES = 128
N_T1 = 160
N_CH = 2
N_COPY = 9 * N_CH + 2

STAGE_OFF = (None, 0, -1, 1, 2)
EVENTS = (("near", 0), ("near", 1), ("opp", 0), ("near", 2), ("near", 3),
          ("opp", 1), ("near", 4), ("opp", 2), ("opp", 3), ("opp", 4))


def stage_units(kind, stage):
    dists = (-1, 1) if kind == "near" else (2,)
    if stage == 0:
        return [(dist, 0) for dist in dists]
    return [(STAGE_OFF[stage], dist) for dist in dists]


UNITS = []
EVENT_START = []
for ev_kind, ev_stage in EVENTS:
    EVENT_START.append(len(UNITS))
    for half_idx in range(2):
        for off in stage_units(ev_kind, ev_stage):
            UNITS.append((half_idx,) + off)


UNIT_INDEX = {unit: pos for pos, unit in enumerate(UNITS)}
SOURCES = ((-1, 0), (1, 0), (0, -1), (0, 1), (-1, -1), (-1, 1), (1, -1), (1, 1),
           (2, 0), (0, 2), (2, -1), (-1, 2), (2, 1), (1, 2), (2, 2))
EVENT_AT = (0, 0, 2, 3, 4, 6, 7, 9, 11, 13)


def flat_view(weight):
    n_layers, d_model, n_heads, head_dim = weight.shape
    split = weight.reshape(n_layers, d_model, n_heads, head_dim // LANES, LANES)
    return split.transpose(0, 1, 3, 2, 4).reshape(n_layers, -1, LANES)


def table(index, values):
    out = jnp.int32(values[0])
    for pos, value in enumerate(values):
        if pos and value != values[0]:
            out = jnp.where(index == pos, jnp.int32(value), out)
    return out


def kernel(n_cp, n_layers, n_heads, head_dim, x_in, wq, wk, wv, wo, out,
           xb, hown, h1, h2, relay, hfull, raw, fs, wc, wob, qb, kb, vb,
           acc, m_st, l_st, obuf, osend, part,
           raw_sem, wo_sem, ls, lr, gs, gr, ds, dr):
    n_tok, d_model = x_in.shape
    n_chip = n_cp // 2
    side = math.isqrt(n_chip)
    half_w = n_heads // 2 * head_dim
    n_ct = head_dim // LANES
    n_t2 = n_tok - N_T1
    quarter = n_tok // 2
    eighth = quarter // 2
    scale = head_dim ** -0.5
    me = lax.axis_index("cp")
    chip = me // 2
    core = me % 2
    other = 1 - core
    px, py = chip % side, chip // side

    def at_xy(x, y):
        return ((y + side) % side) * side + (x + side) % side

    def ring(step):
        return (chip + n_chip + step) % n_chip

    def dev(c, k=None):
        return {"cp": c * 2 + (core if k is None else k)}

    nxt, prv = ring(1), ring(-1)
    xm, xp = at_xy(px - 1, py), at_xy(px + 1, py)
    ym, yp = at_xy(px, py - 1), at_xy(px, py + 1)

    def pass_to(c):
        x, y = c % side, c // side
        return at_xy(x - 1, y + jnp.where(x == 2, 1, 0))

    via = pass_to(chip)
    via_from = at_xy(px + 1, py - jnp.where(px == 1, 1, 0))
    skip_to = (via_from + 2) % n_chip
    skip_from = pass_to(ring(-2))

    barrier = pltpu.get_barrier_semaphore()
    peers = [dev(c) for c in (nxt, prv, xm, xp, ym, yp, via, via_from, skip_to, skip_from)] + [dev(chip, other)]
    for peer in peers:
        pl.semaphore_signal(barrier, inc=1, device_id=peer, device_id_type=pl.DeviceIdType.MESH)

    def raw_copy(layer, i):
        return pltpu.make_async_copy((wq, wk, wv)[i].at[layer], raw.at[i], raw_sem.at[i])

    def wo_copy(layer):
        slot = layer % 2
        return pltpu.make_async_copy(wo.at[layer], wob.at[slot], wo_sem.at[slot])

    for i in range(3):
        raw_copy(0, i).start()
    wo_copy(0).start()
    xb[...] = x_in[...]
    pl.semaphore_wait(barrier, len(peers))

    def convert(layer, which=(0, 1, 2)):
        slot = layer % 2
        d_step = fs.shape[0] // (n_heads * n_ct)
        for i in which:
            raw_copy(layer, i).wait()

            def chunk(j, carry):
                r0 = pl.multiple_of(j * fs.shape[0], fs.shape[0])
                d0 = pl.multiple_of(j * d_step, d_step)
                fs[...] = raw[i, pl.ds(r0, fs.shape[0]), :].astype(F32)
                for hd in range(n_heads // 2):
                    for ct in range(n_ct):
                        first = ct * n_heads + core * (n_heads // 2) + hd
                        piece = fs[pl.ds(first, d_step, stride=n_heads * n_ct), :]
                        wc[slot, i, pl.ds(d0, d_step), pl.ds(hd * head_dim + ct * LANES, LANES)] = piece.astype(BF16)
                return carry
            lax.fori_loop(0, d_model // d_step, chunk, 0)

    def project(rows, slot, which, dst, factor=None):
        for j in range(half_w // head_dim):
            cols = pl.ds(j * head_dim, head_dim)
            val = jnp.dot(rows, wc[slot, which, :, cols], preferred_element_type=F32).astype(BF16)
            if factor is not None:
                val = val * BF16(factor)
            dst[:, cols] = val

    def update(qi, hd, k_ref, v_ref, mask=None, first=False):
        idx = qi * (n_heads // 2) + hd
        cols = pl.ds(hd * head_dim, head_dim)
        s = lax.dot_general(qb[qi, :, cols], k_ref[:, cols], (((1,), (1,)), ((), ())), preferred_element_type=F32)
        if mask is not None:
            s = jnp.where(mask, s, NEG_BIG)
        top = jnp.max(s, axis=1, keepdims=True)
        if first:
            new_m = top
        else:
            old_m = m_st[idx, :, :1]
            new_m = jnp.maximum(old_m, top)
        p = jnp.exp(s - new_m)
        lane_sum = p[:, :LANES]
        for j in range(1, p.shape[1] // LANES):
            lane_sum = lane_sum + p[:, j * LANES:(j + 1) * LANES]
        pv = jnp.dot(p.astype(BF16), v_ref[:, cols], preferred_element_type=F32)
        if first:
            l_st[idx] = lane_sum
            acc[idx] = pv
        else:
            alpha = jnp.exp(old_m - new_m)
            l_st[idx] = l_st[idx] * alpha + lane_sum
            acc[idx] = acc[idx] * alpha + pv
        m_st[idx] = jnp.broadcast_to(new_m, m_st.shape[1:])

    def seg_pos(segs):
        lane = lax.broadcasted_iota(jnp.int32, (1, 2 * n_tok), 1)
        pos = lane
        for start, first_pos in segs:
            pos = jnp.where(lane >= start, lane + (first_pos - start), pos)
        return pos

    def normed(lo=0, n=n_tok):
        xf = xb[lo:lo + n, :].astype(F32)
        return (xf * lax.rsqrt(jnp.mean(xf * xf, axis=-1, keepdims=True) + NORM_EPS)).astype(BF16)

    def o_copy(layer):
        return pltpu.make_async_remote_copy(osend, obuf.at[core], ls.at[layer, N_COPY - 1], lr.at[layer, N_COPY - 1],
                                            device_id=dev(chip, other), device_id_type=pl.DeviceIdType.MESH)

    def out_update(layer, oc):
        slot = layer % 2
        wo_copy(layer).wait()
        wide = d_model // 3
        mine = pl.ds(pl.multiple_of(core * half_w, half_w), half_w)
        theirs = pl.ds(pl.multiple_of(other * half_w, half_w), half_w)
        for j in range(3):
            cols = pl.ds(j * wide, wide)
            part[:, cols] = jnp.dot(obuf[core], wob[slot, mine, cols], preferred_element_type=F32)
        oc.wait_recv()
        for j in range(3):
            cols = pl.ds(j * wide, wide)
            prod = part[:, cols] + jnp.dot(obuf[other], wob[slot, theirs, cols], preferred_element_type=F32)
            xb[:, cols] = (xb[:, cols].astype(F32) + prod).astype(BF16)

    def ici(layer, i, src, dst, c, k=None):
        return pltpu.make_async_remote_copy(src, dst, ls.at[layer, i], lr.at[layer, i],
                                            device_id=dev(c, k), device_id_type=pl.DeviceIdType.MESH)

    def local_layer(layer, carry):
        slot = layer % 2
        c1, c2 = N_T1 // N_CH, n_t2 // N_CH
        mine = pl.ds(pl.multiple_of(core * n_tok, n_tok), n_tok)

        def own_rows(lo, n):
            return hown.at[pl.ds(pl.multiple_of(core * n_tok + lo, 16), n), :]

        def piece(buf, dist, n, ch):
            return buf.at[layer, dist, pl.ds(pl.multiple_of(ch * 2 * n + core * n, 16), n), :]

        chs = range(N_CH)
        near1, far1 = [piece(h1, 0, c1, ch) for ch in chs], [piece(h1, 1, c1, ch) for ch in chs]
        near2, far2 = [piece(h2, 0, c2, ch) for ch in chs], [piece(h2, 1, c2, ch) for ch in chs]
        pass2 = [relay.at[layer, pl.ds(ch * c2, c2), :] for ch in chs]
        t1_own = [ici(layer, ch, own_rows(ch * c1, c1), near1[ch], nxt) for ch in chs]
        t1_fwd = [ici(layer, N_CH + ch, near1[ch], far1[ch], nxt) for ch in chs]
        t2_own = [ici(layer, 2 * N_CH + ch, own_rows(N_T1 + ch * c2, c2), pass2[ch], via) for ch in chs]
        t2_relay = [ici(layer, 3 * N_CH + ch, pass2[ch], far2[ch], skip_to) for ch in chs]
        t2_fwd = [ici(layer, 4 * N_CH + ch, far2[ch], near2[ch], prv) for ch in chs]
        d_n1 = [ici(layer, 5 * N_CH + ch, near1[ch], near1[ch], chip, other) for ch in chs]
        d_f1 = [ici(layer, 6 * N_CH + ch, far1[ch], far1[ch], chip, other) for ch in chs]
        d_n2 = [ici(layer, 7 * N_CH + ch, near2[ch], near2[ch], chip, other) for ch in chs]
        d_f2 = [ici(layer, 8 * N_CH + ch, far2[ch], far2[ch], chip, other) for ch in chs]
        d_own = ici(layer, 9 * N_CH, hown.at[mine], hown.at[mine], chip, other)
        oc = o_copy(layer)

        hown[pl.ds(pl.multiple_of(core * n_tok, n_tok), N_T1), :] = normed(0, N_T1)
        for cp in t1_own:
            cp.start()
        hown[pl.ds(pl.multiple_of(core * n_tok + N_T1, 16), n_t2), :] = normed(N_T1, n_t2)
        for cp in t2_own:
            cp.start()
        d_own.start()
        wo_copy(layer + 1).start()

        @pl.when(layer == 0)
        def _():
            convert(0)
            for i in range(3):
                raw_copy(1, i).start()

        def own_block(b):
            dst_rows = pl.ds(pl.multiple_of(b * n_tok, n_tok), n_tok)
            rows = hown[dst_rows, :]
            project(rows, slot, 0, qb.at[b], scale)
            project(rows, slot, 1, kb.at[0, dst_rows])
            project(rows, slot, 2, vb.at[0, dst_rows])

        def take(arrived, onward, side_copy):
            arrived.wait_recv()
            if onward is not None:
                onward.start()
            if side_copy is not None:
                side_copy.start()

        def kv_rows(buf, dist, lo, n, dst_lo):
            rows = buf[layer, dist, lo:lo + n]
            project(rows, slot, 1, kb.at[1 + dist, pl.ds(dst_lo + lo, n)])
            project(rows, slot, 2, vb.at[1 + dist, pl.ds(dst_lo + lo, n)])

        own_block(core)
        d_own.wait_recv()
        own_block(other)
        row_i = lax.broadcasted_iota(jnp.int32, (n_tok, 1), 0)
        lane_i = lax.broadcasted_iota(jnp.int32, (1, 2 * n_tok), 1)
        for hd in range(n_heads // 2):
            update(0, hd, kb.at[0, :n_tok], vb.at[0, :n_tok], lane_i[:, :n_tok] <= row_i, first=True)
            update(1, hd, kb.at[0], vb.at[0], lane_i <= row_i + n_tok, first=True)
        convert(layer + 1, (0,))
        take(t2_own[0], t2_relay[0], None)
        convert(layer + 1, (1,))
        take(t1_own[0], t1_fwd[0], d_n1[0])
        convert(layer + 1, (2,))

        @pl.when(layer + 2 < n_layers)
        def _():
            for i in range(3):
                raw_copy(layer + 2, i).start()

        for ch in range(1, N_CH):
            take(t2_own[ch], t2_relay[ch], None)
        for ch in range(1, N_CH):
            take(t1_own[ch], t1_fwd[ch], d_n1[ch])
        take(t2_relay[0], t2_fwd[0], d_f2[0])
        for ch in chs:
            d_n1[ch].wait_recv()

        @pl.when(chip >= 1)
        def _():
            kv_rows(h1, 0, 0, 2 * N_T1, 0)
        for ch in range(1, N_CH):
            take(t2_relay[ch], t2_fwd[ch], d_f2[ch])
        for ch in chs:
            d_f2[ch].wait_recv()

        @pl.when(chip >= 2)
        def _():
            kv_rows(h2, 1, 0, 2 * n_t2, 2 * N_T1)
        for ch in range(N_CH - 1):
            take(t1_fwd[ch], None, d_f1[ch])
            take(t2_fwd[ch], None, d_n2[ch])
        for ch in range(N_CH - 1):
            d_f1[ch].wait_recv()

        @pl.when(chip >= 2)
        def _():
            kv_rows(h1, 1, 0, 2 * (N_T1 - c1), 0)
        take(t2_fwd[N_CH - 1], None, d_n2[N_CH - 1])
        for ch in chs:
            d_n2[ch].wait_recv()

        @pl.when(chip >= 1)
        def _():
            kv_rows(h2, 0, 0, 2 * n_t2, 2 * N_T1)
        take(t1_fwd[N_CH - 1], None, d_f1[N_CH - 1])

        @pl.when(chip >= 1)
        def _():
            for qi in range(2):
                for hd in range(n_heads // 2):
                    update(qi, hd, kb.at[1], vb.at[1])
        d_f1[N_CH - 1].wait_recv()

        @pl.when(chip >= 2)
        def _():
            kv_rows(h1, 1, 2 * (N_T1 - c1), 2 * c1, 0)
            segs = [(ch * 2 * c1 + k * c1, k * n_tok + ch * c1) for ch in chs for k in range(2)]
            segs += [(2 * N_T1 + ch * 2 * c2 + k * c2, k * n_tok + N_T1 + ch * c2) for ch in chs for k in range(2)]
            key_pos = seg_pos(segs)
            for qi in range(2):
                for hd in range(n_heads // 2):
                    update(qi, hd, kb.at[2], vb.at[2], row_i + ((qi + 4) * n_tok - WINDOW) < key_pos)

        def put(qi, dst):
            for hd in range(n_heads // 2):
                idx = qi * (n_heads // 2) + hd
                row_sum = jnp.sum(l_st[idx], axis=1, keepdims=True)
                dst[:, pl.ds(hd * head_dim, head_dim)] = (acc[idx] / row_sum).astype(BF16)

        put(other, osend)
        oc.start()
        put(core, obuf.at[core])
        out_update(layer, oc)
        for group in (t1_own, t1_fwd, t2_own, t2_relay, t2_fwd, d_n1, d_f1, d_n2, d_f2, [d_own, oc]):
            for cp in group:
                cp.wait_send()
        return carry

    lax.fori_loop(0, n_layers - 1, local_layer, 0)

    last = n_layers - 1
    slot = last % 2
    h_new = normed()
    mine = pl.ds(pl.multiple_of(core * quarter, quarter), quarter)
    for hf in range(2):
        hfull[chip * 2 + hf, mine, :] = h_new[hf * quarter:(hf + 1) * quarter]

    def chip_off(hf, dp, dsec):
        if hf == 0:
            return at_xy(px + dp, py + dsec)
        return at_xy(px + dsec, py + dp)

    def stage_chip(hf, stage, dist):
        if stage == 0:
            return chip_off(hf, dist, 0)
        return chip_off(hf, STAGE_OFF[stage], dist)

    def stage_peer(hf, stage, dist):
        if stage == 0:
            return chip_off(hf, dist, 0)
        return chip_off(hf, 0, dist)

    def g_rows(c, hf, lo, n):
        return hfull.at[c * 2 + hf, pl.ds(pl.multiple_of(core * quarter + lo, 16), n), :]

    def g_copy(hf, stage, kind):
        sgn = 1 if kind % 2 == 0 else -1
        if kind < 2:
            ref = g_rows(stage_chip(hf, stage, 0), hf, 0, quarter)
        else:
            ref = g_rows(stage_chip(hf, stage, -sgn), hf, 0 if kind == 2 else eighth, eighth)
        i = (hf * 5 + stage) * 4 + kind
        return pltpu.make_async_remote_copy(ref, ref, gs.at[i], gr.at[i], device_id=dev(stage_peer(hf, stage, sgn)),
                                            device_id_type=pl.DeviceIdType.MESH)

    def d_copy(i, c, hf):
        ref = g_rows(c, hf, 0, quarter)
        return pltpu.make_async_remote_copy(ref, ref, ds.at[i], dr.at[i], device_id=dev(chip, other),
                                            device_id_type=pl.DeviceIdType.MESH)

    for stage in range(2):
        for hf in range(2):
            for kind in range(2):
                g_copy(hf, stage, kind).start()
    n_units = len(UNITS)
    for hf in range(2):
        d_copy(n_units + hf, chip, hf).start()

    for hf in range(2):
        d_copy(n_units + hf, chip, hf).wait_recv()
        rows = hfull[chip * 2 + hf]
        seg = pl.ds(hf * n_tok, n_tok)
        project(rows, slot, 0, qb.at[hf], scale)
        project(rows, slot, 1, kb.at[0, seg])
        project(rows, slot, 2, vb.at[0, seg])
    key_pos = seg_pos([(hf * n_tok + k * quarter, k * n_tok + hf * quarter) for hf in range(2) for k in range(2)])
    row_i = lax.broadcasted_iota(jnp.int32, (n_tok, 1), 0)
    for qi in range(2):
        query_pos = jnp.where(row_i >= quarter, row_i + (n_tok - quarter), row_i) + qi * quarter
        for hd in range(n_heads // 2):
            update(qi, hd, kb.at[0], vb.at[0], key_pos <= query_pos, first=True)

    def run_event(e):
        kind, stage = EVENTS[e]
        at = EVENT_START[e]
        for hf in range(2):
            offs = stage_units(kind, stage)
            if kind == "near":
                for knd in range(2):
                    g_copy(hf, stage, knd).wait_recv()
                for knd in range(2, 4):
                    g_copy(hf, stage, knd).start()
                if stage == 0:
                    for nstage in (2, 3):
                        for knd in range(2):
                            g_copy(hf, nstage, knd).start()
            else:
                for knd in range(2, 4):
                    g_copy(hf, stage, knd).wait_recv()
                if stage == 0:
                    for knd in range(2):
                        g_copy(hf, 4, knd).start()
            for off in offs:
                d_copy(at, chip_off(hf, *off), hf).start()
                at += 1

    def source_step(i, carry):
        for e in range(len(EVENTS)):
            @pl.when(i == EVENT_AT[e])
            def _():
                run_event(e)
        dx = table(i, [off[0] for off in SOURCES])
        dy = table(i, [off[1] for off in SOURCES])
        src = at_xy(px + dx, py + dy)
        for hf in range(2):
            unit = table(i, [UNIT_INDEX[(hf,) + (off if hf == 0 else off[::-1])] for off in SOURCES])
            d_copy(unit, src, hf).wait_recv()

        @pl.when(src < chip)
        def _():
            rows = hfull[pl.ds(src * 2, 2)].reshape(2 * n_tok, d_model)
            project(rows, slot, 1, kb.at[1])
            project(rows, slot, 2, vb.at[1])
            for qi in range(2):
                for hd in range(n_heads // 2):
                    update(qi, hd, kb.at[1], vb.at[1])
        return carry

    lax.fori_loop(0, len(SOURCES), source_step, 0)

    def put_rows(c, dst):
        seg = pl.ds(pl.multiple_of(c * quarter, quarter), quarter)
        for qi in range(2):
            for hd in range(n_heads // 2):
                idx = qi * (n_heads // 2) + hd
                val = acc[idx, seg, :] / jnp.sum(l_st[idx, seg, :], axis=1, keepdims=True)
                dst[qi * quarter:(qi + 1) * quarter, pl.ds(hd * head_dim, head_dim)] = val.astype(BF16)

    put_rows(other, osend)
    oc = o_copy(last)
    oc.start()
    put_rows(core, obuf.at[core])
    out_update(last, oc)
    out[...] = xb[...]
    oc.wait_send()
    for hf in range(2):
        for stage in range(5):
            for kind in range(4):
                g_copy(hf, stage, kind).wait_send()
        d_copy(n_units + hf, chip, hf).wait_send()
    for i in range(n_units):
        hf = UNITS[i][0]
        d_copy(i, chip_off(hf, *UNITS[i][1:]), hf).wait_send()


def solution(mesh):
    n_cp = mesh.shape["cp"]

    def device_body(hidden, w_query, w_key, w_value, w_out):
        n_tok, d_model = hidden.shape
        n_layers, n_heads, head_dim, _ = w_out.shape
        half_w = n_heads // 2 * head_dim
        n_loc = n_layers - 1
        n_t2 = n_tok - N_T1
        flat = n_heads * head_dim // LANES * d_model
        vmem = pl.BlockSpec(memory_space=pltpu.VMEM)
        hbm = pl.BlockSpec(memory_space=pl.ANY)
        scratch = [
            pltpu.VMEM((n_tok, d_model), BF16),
            pltpu.VMEM((2 * n_tok, d_model), BF16),
            pltpu.VMEM((n_loc, 2, 2 * N_T1, d_model), BF16),
            pltpu.VMEM((n_loc, 2, 2 * n_t2, d_model), BF16),
            pltpu.VMEM((n_loc, n_t2, d_model), BF16),
            pltpu.VMEM((n_cp, n_tok, d_model), BF16),
            pltpu.VMEM((3, flat, LANES), BF16),
            pltpu.VMEM((n_heads * head_dim, LANES), F32),
            pltpu.VMEM((2, 3, d_model, half_w), BF16),
            pltpu.VMEM((2, n_heads * head_dim, d_model), BF16),
            pltpu.VMEM((2, n_tok, half_w), BF16),
            pltpu.VMEM((3, 2 * n_tok, half_w), BF16),
            pltpu.VMEM((3, 2 * n_tok, half_w), BF16),
            pltpu.VMEM((n_heads, n_tok, head_dim), F32),
            pltpu.VMEM((n_heads, n_tok, LANES), F32),
            pltpu.VMEM((n_heads, n_tok, LANES), F32),
            pltpu.VMEM((2, n_tok, half_w), BF16),
            pltpu.VMEM((n_tok, half_w), BF16),
            pltpu.VMEM((n_tok, d_model), F32),
            pltpu.SemaphoreType.DMA((3,)),
            pltpu.SemaphoreType.DMA((2,)),
            pltpu.SemaphoreType.DMA((n_layers, N_COPY)),
            pltpu.SemaphoreType.DMA((n_layers, N_COPY)),
            pltpu.SemaphoreType.DMA((40,)),
            pltpu.SemaphoreType.DMA((40,)),
            pltpu.SemaphoreType.DMA((len(UNITS) + 2,)),
            pltpu.SemaphoreType.DMA((len(UNITS) + 2,)),
        ]
        return pl.pallas_call(
            functools.partial(kernel, n_cp, n_layers, n_heads, head_dim),
            out_shape=jax.ShapeDtypeStruct(hidden.shape, hidden.dtype),
            in_specs=[vmem, hbm, hbm, hbm, hbm],
            out_specs=vmem,
            scratch_shapes=scratch,
            compiler_params=pltpu.CompilerParams(collective_id=0, has_side_effects=True, vmem_limit_bytes=66_500_000),
        )(hidden, flat_view(w_query), flat_view(w_key), flat_view(w_value),
          w_out.reshape(n_layers, n_heads * head_dim, d_model))

    row_spec = P(("dp", "cp"), None)
    return jax.shard_map(device_body, mesh=mesh, in_specs=(row_spec, P(), P(), P(), P()), out_specs=row_spec, check_vma=False)
```

```python
import functools
import math

import jax
import jax.numpy as jnp
from jax import lax
from jax.experimental import pallas as pl
from jax.experimental.pallas import tpu as pltpu
from jax.sharding import PartitionSpec as P

WINDOW = 1024
NORM_EPS = 1e-6
NEG_BIG = -1e30
BF16 = jnp.bfloat16
F32 = jnp.float32
LANES = 128
N_T1 = 160
PIECE = 32
N_1 = N_T1 // PIECE

BLOCKS = ((0, 1), (0, 3), (0, 2), (1, 1), (1, 3), (3, 1), (3, 3), (1, 2), (2, 1), (2, 3), (3, 2), (2, 2))
ARRIVE_AT = {("y", 1): 0, ("y", 3): 2, ("opp", 1): 4, ("y", 2): 6, ("opp", 3): 8, ("opp", 2): 9}


def flat_view(weight):
    n_layers, d_model, n_heads, head_dim = weight.shape
    split = weight.reshape(n_layers, d_model, n_heads, head_dim // LANES, LANES)
    return split.transpose(0, 1, 3, 2, 4).reshape(n_layers, -1, LANES)


def table(index, values):
    out = jnp.int32(values[0])
    for pos, value in enumerate(values):
        if pos and value != values[0]:
            out = jnp.where(index == pos, jnp.int32(value), out)
    return out


def kernel(n_cp, n_layers, n_heads, head_dim, x_in, wq, wk, wv, wo, out,
           xb, hown, hh, tk, relay, kvg, st, qst, qg, og, raw, fs, wc, wob, qt, kb, vb,
           acc, m_st, l_st, obuf, osend, part,
           raw_sem, wo_sem, ls, lr, st_s, kv_r, q_r, ys, yr, ds, dr, o_s, o_r):
    n_tok, d_model = x_in.shape
    n_chip = n_cp // 2
    side = math.isqrt(n_chip)
    half_w = n_heads // 2 * head_dim
    n_ct = head_dim // LANES
    n_t2 = n_tok - N_T1
    scale = head_dim ** -0.5
    me = lax.axis_index("cp")
    chip = me // 2
    core = me % 2
    other = 1 - core
    px, py = chip % side, chip // side

    def at_xy(x, y):
        return ((y + side) % side) * side + (x + side) % side

    def ring(step):
        return (chip + n_chip + step) % n_chip

    def dev(c, k=None):
        return {"cp": c * 2 + (core if k is None else k)}

    nxt, prv = ring(1), ring(-1)
    xm, xp = at_xy(px - 1, py), at_xy(px + 1, py)
    ym, yp = at_xy(px, py - 1), at_xy(px, py + 1)

    def pass_to(c):
        x, y = c % side, c // side
        return at_xy(x - 1, y + jnp.where(x == 2, 1, 0))

    via = pass_to(chip)
    via_from = at_xy(px + 1, py - jnp.where(px == 1, 1, 0))
    skip_to = (via_from + 2) % n_chip
    skip_from = pass_to(ring(-2))

    barrier = pltpu.get_barrier_semaphore()
    peers = [dev(c) for c in (nxt, prv, ym, yp, via, via_from, skip_to, skip_from)] + [dev(chip, other)]
    peers += [dev(at_xy(px + d, py), k) for d in range(1, side) for k in range(2)]
    for peer in peers:
        pl.semaphore_signal(barrier, inc=1, device_id=peer, device_id_type=pl.DeviceIdType.MESH)

    def raw_copy(layer, i):
        return pltpu.make_async_copy((wq, wk, wv)[i].at[layer], raw.at[i], raw_sem.at[i])

    def wo_copy(layer):
        slot = layer % 2
        return pltpu.make_async_copy(wo.at[layer], wob.at[slot], wo_sem.at[slot])

    for i in range(3):
        raw_copy(0, i).start()
    wo_copy(0).start()
    xb[...] = x_in[...]

    def convert(layer, which=(0, 1, 2)):
        slot = layer % 2
        d_step = fs.shape[0] // (n_heads * n_ct)
        for i in which:
            raw_copy(layer, i).wait()

            def chunk(j, carry):
                r0 = pl.multiple_of(j * fs.shape[0], fs.shape[0])
                d0 = pl.multiple_of(j * d_step, d_step)
                fs[...] = raw[i, pl.ds(r0, fs.shape[0]), :].astype(F32)
                for hd in range(n_heads // 2):
                    for ct in range(n_ct):
                        first = ct * n_heads + core * (n_heads // 2) + hd
                        piece = fs[pl.ds(first, d_step, stride=n_heads * n_ct), :]
                        wc[slot, i, pl.ds(d0, d_step), pl.ds(hd * head_dim + ct * LANES, LANES)] = piece.astype(BF16)
                return carry
            lax.fori_loop(0, d_model // d_step, chunk, 0)

    def project(rows, slot, which, dst):
        for j in range(half_w // head_dim):
            cols = pl.ds(j * head_dim, head_dim)
            dst[:, cols] = jnp.dot(rows, wc[slot, which, :, cols], preferred_element_type=F32).astype(BF16)

    def project_q(rows, slot, q_cols):
        for j in range(half_w // head_dim):
            cols = pl.ds(j * head_dim, head_dim)
            val = jnp.dot(rows, wc[slot, 0, :, cols], preferred_element_type=F32).astype(BF16)
            qt[cols, q_cols] = (val * BF16(scale)).T

    def soft_step(k_val, q_val, v_val, hd, q_cols, mask=None, first=False):
        s = jnp.dot(k_val, q_val, preferred_element_type=F32)
        if mask is not None:
            s = jnp.where(mask, s, NEG_BIG)
        new_m = jnp.max(s, axis=0, keepdims=True)
        if not first:
            old_m = m_st[hd, :1, q_cols]
            new_m = jnp.maximum(old_m, new_m)
        p = jnp.exp(s - new_m)
        part_sum = jnp.sum(p.reshape(p.shape[0] // 8, 8, p.shape[1]), axis=0)
        pv = lax.dot_general(v_val, p.astype(BF16), (((0,), (0,)), ((), ())), preferred_element_type=F32)
        if first:
            l_st[hd, :, q_cols] = part_sum
            acc[hd, :, q_cols] = pv
        else:
            alpha = jnp.exp(old_m - new_m)
            l_st[hd, :, q_cols] = l_st[hd, :, q_cols] * alpha + part_sum
            acc[hd, :, q_cols] = acc[hd, :, q_cols] * alpha + pv
        m_st[hd, :1, q_cols] = new_m

    def update(qi, hd, k_ref, v_ref, mask=None, first=False):
        dims = pl.ds(hd * head_dim, head_dim)
        q_cols = pl.ds(qi * n_tok, n_tok)
        soft_step(k_ref[:, dims], qt[dims, q_cols], v_ref[:, dims], hd, q_cols, mask, first)

    def update_all(k_ref, v_ref, mask_of=None):
        for qi in range(2):
            mask = None if mask_of is None else mask_of(qi)
            for hd in range(n_heads // 2):
                update(qi, hd, k_ref, v_ref, mask)

    def output_rows(hd, q_cols):
        total = jnp.sum(l_st[hd, :, q_cols], axis=0, keepdims=True)
        return (acc[hd, :, q_cols] / total).astype(BF16).T

    def normed(lo=0, n=n_tok):
        xf = xb[lo:lo + n, :].astype(F32)
        return (xf * lax.rsqrt(jnp.mean(xf * xf, axis=-1, keepdims=True) + NORM_EPS)).astype(BF16)

    def o_copy(layer):
        return pltpu.make_async_remote_copy(osend, obuf.at[core], ls.at[layer, ls.shape[1] - 1], lr.at[layer, lr.shape[1] - 1],
                                            device_id=dev(chip, other), device_id_type=pl.DeviceIdType.MESH)

    def out_own(layer):
        slot = layer % 2
        wo_copy(layer).wait()
        wide = d_model // 3
        mine = pl.ds(pl.multiple_of(core * half_w, half_w), half_w)
        for j in range(3):
            cols = pl.ds(j * wide, wide)
            part[:, cols] = jnp.dot(obuf[core], wob[slot, mine, cols], preferred_element_type=F32)

    def out_other(layer, lo, n):
        slot = layer % 2
        wide = d_model // 3
        theirs = pl.ds(pl.multiple_of(other * half_w, half_w), half_w)
        for j in range(3):
            cols = pl.ds(j * wide, wide)
            prod = part[lo:lo + n, cols] + jnp.dot(obuf[other, lo:lo + n, :], wob[slot, theirs, cols], preferred_element_type=F32)
            xb[lo:lo + n, cols] = (xb[lo:lo + n, cols].astype(F32) + prod).astype(BF16)

    def ici(layer, i, src, dst, c, k=None):
        return pltpu.make_async_remote_copy(src, dst, ls.at[layer, i], lr.at[layer, i],
                                            device_id=dev(c, k), device_id_type=pl.DeviceIdType.MESH)

    n_2 = n_t2 // PIECE
    both = 2 * PIECE
    off_near1 = [ch * both for ch in range(N_1)]
    off_far2 = [2 * N_T1 + ch * both for ch in range(n_2)]
    off_near2, off_far1, groups = [], [], []
    at_row = 2 * n_tok
    per = -(-N_1 // n_2)
    for ch in range(n_2):
        first = at_row
        off_near2.append(at_row)
        at_row += both
        far_ids = list(range(ch * per, min(N_1, (ch + 1) * per)))
        for _ in far_ids:
            off_far1.append(at_row)
            at_row += both
        groups.append((first, at_row - first, far_ids))
    key_i = lax.broadcasted_iota(jnp.int32, tk.shape, 0)
    limit = jnp.full(tk.shape, 4 * n_tok, jnp.int32)
    for offs, base in ((off_far1, 0), (off_far2, N_T1)):
        for ch, off in enumerate(offs):
            for k in range(2):
                start = off + k * PIECE
                inside = (key_i >= start) & (key_i < start + PIECE)
                shift = k * n_tok + base + ch * PIECE + WINDOW - 4 * n_tok - start
                limit = jnp.where(inside, jnp.where(chip >= 2, key_i + shift, -1), limit)
    tk[...] = limit

    mine = pl.ds(pl.multiple_of(core * n_tok, n_tok), n_tok)

    def own_rows(lo, n):
        return hown.at[pl.ds(pl.multiple_of(core * n_tok + lo, 16), n), :]

    def own_copies(layer):
        hl = hh.at[layer]
        t1 = [ici(layer, ch, own_rows(ch * PIECE, PIECE), hl.at[piece_rows(off), :], nxt) for ch, off in enumerate(off_near1)]
        t2 = [ici(layer, N_1 + ch, own_rows(N_T1 + ch * PIECE, PIECE), relay.at[layer, pl.ds(ch * PIECE, PIECE), :], via)
              for ch in range(n_2)]
        side_own = ici(layer, N_1 + n_2, hown.at[mine], hown.at[mine], chip, other)
        return t1, t2, side_own

    def piece_rows(off):
        return pl.ds(pl.multiple_of(off + core * PIECE, 16), PIECE)

    def launch1():
        hown[pl.ds(pl.multiple_of(core * n_tok, n_tok), N_T1), :] = normed(0, N_T1)

    def launch2():
        hown[pl.ds(pl.multiple_of(core * n_tok + N_T1, 16), n_t2), :] = normed(N_T1, n_t2)

    def local_layer(layer, carry):
        slot = layer % 2
        t1_own, t2_own, d_own = own_copies(layer)
        base = N_1 + n_2 + 1

        def piece(off):
            return hh.at[layer, piece_rows(off), :]

        near1, far1 = [piece(off) for off in off_near1], [piece(off) for off in off_far1]
        near2, far2 = [piece(off) for off in off_near2], [piece(off) for off in off_far2]
        pass2 = [relay.at[layer, pl.ds(ch * PIECE, PIECE), :] for ch in range(n_2)]

        def series(srcs, dsts, c, k=None):
            nonlocal base
            out = [ici(layer, base + i, a, b, c, k) for i, (a, b) in enumerate(zip(srcs, dsts))]
            base += len(out)
            return out

        t1_fwd = series(near1, far1, nxt)
        t2_relay = series(pass2, far2, skip_to)
        t2_fwd = series(far2, near2, prv)
        d_n1 = series(near1, near1, chip, other)
        d_f1 = series(far1, far1, chip, other)
        d_n2 = series(near2, near2, chip, other)
        d_f2 = series(far2, far2, chip, other)
        oc = o_copy(layer)

        @pl.when(layer == 0)
        def _():
            launch1()
            pl.semaphore_wait(barrier, len(peers))
            for cp in t1_own:
                cp.start()
            launch2()
            for cp in t2_own:
                cp.start()
            d_own.start()
            convert(0)
            for i in range(3):
                raw_copy(1, i).start()
        wo_copy(layer + 1).start()

        def own_block(b):
            dst_rows = pl.ds(pl.multiple_of(b * n_tok, n_tok), n_tok)
            rows = hown[dst_rows, :]
            project_q(rows, slot, dst_rows)
            project(rows, slot, 1, kb.at[dst_rows])
            project(rows, slot, 2, vb.at[dst_rows])

        def take(arrived, onward, side_copy):
            arrived.wait_recv()
            if onward is not None:
                onward.start()
            if side_copy is not None:
                side_copy.start()

        def take_n1(ch):
            take(t1_own[ch], t1_fwd[ch], d_n1[ch])

        def take_pass(ch):
            take(t2_own[ch], t2_relay[ch], None)

        def take_f2(ch):
            take(t2_relay[ch], t2_fwd[ch], d_f2[ch])

        def take_late(g):
            for ch in groups[g][2]:
                take(t1_fwd[ch], None, d_f1[ch])
            take(t2_fwd[g], None, d_n2[g])

        def side_late(g):
            for ch in groups[g][2]:
                d_f1[ch].wait_recv()
            d_n2[g].wait_recv()

        def kv_rows(lo, n):
            @pl.when(chip >= 1)
            def _():
                rows = hh[layer, lo:lo + n]
                project(rows, slot, 1, kb.at[pl.ds(2 * n_tok + lo, n)])
                project(rows, slot, 2, vb.at[pl.ds(2 * n_tok + lo, n)])

        lane_i = lax.broadcasted_iota(jnp.int32, (1, n_tok), 1)

        def attend(lo, n):
            def mask_of(qi):
                rows = tk[lo:lo + n, :]
                return jnp.concatenate([rows] * (n_tok // LANES), axis=1) > lane_i + qi * n_tok

            @pl.when(chip >= 1)
            def _():
                at = pl.ds(2 * n_tok + lo, n)
                update_all(kb.at[at], vb.at[at], mask_of)

        own_block(core)
        d_own.wait_recv()
        own_block(other)
        row_i = lax.broadcasted_iota(jnp.int32, (2 * n_tok, n_tok), 0)
        col_i = lax.broadcasted_iota(jnp.int32, (2 * n_tok, n_tok), 1)
        for hd in range(n_heads // 2):
            update(0, hd, kb.at[:n_tok], vb.at[:n_tok], row_i[:n_tok] <= col_i[:n_tok], first=True)
            update(1, hd, kb.at[:2 * n_tok], vb.at[:2 * n_tok], row_i <= col_i + n_tok, first=True)
        for ch in range(min(3, n_2)):
            take_pass(ch)
            take_n1(ch)
            convert(layer + 1, (ch,))

        @pl.when(layer + 2 < n_layers)
        def _():
            for i in range(3):
                raw_copy(layer + 2, i).start()

        take_n1(3)
        take_f2(0)
        take_n1(4)
        take_f2(1)
        for ch in range(N_1):
            d_n1[ch].wait_recv()
        kv_rows(0, 2 * N_T1)
        take_f2(2)
        for ch in range(n_2):
            d_f2[ch].wait_recv()
        kv_rows(2 * N_T1, 2 * n_t2)
        take_late(0)
        attend(0, 2 * n_tok)
        for g in range(n_2):
            side_late(g)
            if g == n_2 - 2:
                take_late(g + 1)
            kv_rows(*groups[g][:2])
            if g < n_2 - 2:
                take_late(g + 1)
            attend(*groups[g][:2])

        def put(qi, dst):
            for hd in range(n_heads // 2):
                dst[:, pl.ds(hd * head_dim, head_dim)] = output_rows(hd, pl.ds(pl.multiple_of(qi * n_tok, n_tok), n_tok))

        put(other, osend)
        oc.start()
        put(core, obuf.at[core])
        out_own(layer)
        for group in (t1_own, t1_fwd, t2_own, t2_relay, t2_fwd, d_n1, d_f1, d_n2, d_f2, [d_own]):
            for cp in group:
                cp.wait_send()
        oc.wait_recv()
        go_on = layer + 1 < n_layers - 1
        later1, later2, later_own = own_copies(layer + 1)
        out_other(layer, 0, N_T1)

        @pl.when(go_on)
        def _():
            launch1()
            for cp in later1:
                cp.start()
        out_other(layer, N_T1, n_t2)

        @pl.when(go_on)
        def _():
            launch2()
            for cp in later2:
                cp.start()
            later_own.start()
        oc.wait_send()
        return carry

    lax.fori_loop(0, n_layers - 1, local_layer, 0)

    last = n_layers - 1
    slot = last % 2
    per_core = n_heads // 2
    main = core == px // per_core
    launch1()
    launch2()
    d_own = ici(last, 0, hown.at[mine], hown.at[mine], chip, other)
    d_own.start()
    m_st[...] = jnp.full(m_st.shape, NEG_BIG, F32)
    l_st[...] = jnp.zeros(l_st.shape, F32)
    acc[...] = jnp.zeros(acc.shape, F32)

    def rcopy(src, dst, send_sem, recv_sem, target):
        return pltpu.make_async_remote_copy(src, dst, send_sem, recv_sem, device_id=target, device_id_type=pl.DeviceIdType.MESH)

    def rel_to(hd):
        return (px - hd + side) % side

    def heads():
        return [(j, core * per_core + j) for j in range(per_core)]

    def kv_send(j, hd):
        return rcopy(st.at[j], kvg.at[chip], st_s.at[j], kv_r.at[rel_to(hd)], dev(at_xy(hd, py)))

    def q_send(j, hd, k):
        i = per_core + 2 * j + k
        return rcopy(qst.at[j, k], qg.at[px], st_s.at[i], q_r.at[rel_to(hd)], dev(at_xy(hd, py), k))

    def q_side(j):
        i = per_core + 2 * per_core + j
        return rcopy(qst.at[j, other], qg.at[px], st_s.at[i], q_r.at[0], dev(chip, other))

    def block_chip(dx, dy):
        return at_xy(px + dx, py + dy)

    def y_copy(dx, kind):
        if kind < 2:
            ref = kvg.at[block_chip(dx, 0)]
        else:
            ref = kvg.at[block_chip(dx, -1 if kind == 2 else 1), kind - 2]
        i = dx * 4 + kind
        return rcopy(ref, ref, ys.at[i], yr.at[i], dev(yp if kind % 2 == 0 else ym))

    def to_side(dx, dy):
        ref = kvg.at[block_chip(dx, dy)]
        i = dx * side + dy
        return rcopy(ref, ref, ds.at[i], dr.at[i], dev(chip, other))

    def own_kv(b):
        seg = pl.ds(pl.multiple_of(b * n_tok, n_tok), n_tok)
        rows = hown[seg, :]
        for j in range(per_core):
            cols = pl.ds(j * head_dim, head_dim)
            for i in range(2):
                st[j, i, seg, :] = jnp.dot(rows, wc[slot, 1 + i, :, cols], preferred_element_type=F32).astype(BF16)

    def own_q(b):
        rows = hown[pl.ds(pl.multiple_of(b * n_tok, n_tok), n_tok), :]
        for j in range(per_core):
            cols = pl.ds(j * head_dim, head_dim)
            val = jnp.dot(rows, wc[slot, 0, :, cols], preferred_element_type=F32).astype(BF16)
            qst[j, b] = (val * BF16(scale)).T

    own_kv(core)
    d_own.wait_recv()
    own_kv(other)
    for j, hd in heads():
        @pl.when(hd == px)
        def _():
            kvg[chip] = st[j]
            y_copy(0, 0).start()
            y_copy(0, 1).start()
            to_side(0, 0).start()

        @pl.when(hd != px)
        def _():
            kv_send(j, hd).start()
    own_q(core)
    own_q(other)
    for j, hd in heads():
        @pl.when(hd == px)
        def _():
            q_side(j).start()
            qg[px] = qst[j, core]

        @pl.when(hd != px)
        def _():
            for k in range(2):
                q_send(j, hd, k).start()

    def arrive(what, dx):
        @pl.when(main)
        def _():
            if what == "row":
                rcopy(st.at[0], kvg.at[block_chip(dx, 0)], st_s.at[0], kv_r.at[dx], dev(chip, other)).wait_recv()
                y_copy(dx, 0).start()
                y_copy(dx, 1).start()
                to_side(dx, 0).start()
            elif what == "y":
                for kind in range(2):
                    y_copy(dx, kind).wait_recv()
                for kind in range(2, 4):
                    y_copy(dx, kind).start()
                to_side(dx, side - 1).start()
                to_side(dx, 1).start()
            else:
                for kind in range(2, 4):
                    rcopy(kvg.at[block_chip(dx, 2), kind - 2], kvg.at[block_chip(dx, 2), kind - 2], ys.at[dx * 4 + kind],
                          yr.at[dx * 4 + kind], dev(chip, other)).wait_recv()
                to_side(dx, 2).start()

    def have(dx, dy, i):
        @pl.when(jnp.logical_not(main))
        def _():
            c = block_chip(dx, dy)
            rcopy(kvg.at[c], kvg.at[c], ds.at[i], dr.at[i], dev(chip, other)).wait_recv()

    arrive("y", 0)
    arrive("row", 1)
    arrive("row", side - 1)
    arrive("opp", 0)
    arrive("row", 2)
    for dx in range(side):
        q_in = rcopy(qst.at[0, 0], qg.at[(px + dx) % side], st_s.at[0], q_r.at[dx], dev(chip, other))
        if dx == 0:
            @pl.when(jnp.logical_not(main))
            def _():
                q_in.wait_recv()
        else:
            q_in.wait_recv()

    def q_cols_of(b):
        return pl.ds(pl.multiple_of(b % 2 * n_tok, n_tok), n_tok)

    key_i = lax.broadcasted_iota(jnp.int32, (2 * n_tok, n_tok), 0)
    query_i = lax.broadcasted_iota(jnp.int32, (2 * n_tok, n_tok), 1) + core * n_tok

    def row_step(dx, carry):
        src_x = (px + dx) % side
        have(dx, 0, dx * side)
        c = block_chip(dx, 0)

        def one(b, c2):
            @pl.when(src_x <= b)
            def _():
                mask = key_i - query_i <= (b - src_x) * (2 * n_tok)
                soft_step(kvg[c, 0], qg[b], kvg[c, 1], b // 2, q_cols_of(b), mask)
            return c2

        lax.fori_loop(0, side, one, 0)
        return carry

    lax.fori_loop(0, side, row_step, 0)

    def block_step(i, carry):
        for (what, col), when in ARRIVE_AT.items():
            @pl.when(i == when)
            def _():
                arrive(what, col)
        dx = table(i, [blk[0] for blk in BLOCKS])
        dy = table(i, [blk[1] for blk in BLOCKS])
        have(dx, dy, dx * side + dy)
        c = block_chip(dx, dy)

        @pl.when(c // side < py)
        def _():
            for b in range(side):
                soft_step(kvg[c, 0], qg[b], kvg[c, 1], b // 2, pl.ds(b % 2 * n_tok, n_tok))
        return carry

    lax.fori_loop(0, len(BLOCKS), block_step, 0)

    def o_send(rel):
        b = (px + rel) % side
        return rcopy(qst.at[rel // 2, rel % 2], og.at[px], o_s.at[rel], o_r.at[rel], dev(at_xy(px + rel, py)))

    def o_in(rel):
        ref = og.at[(px - rel + side) % side]
        return rcopy(ref, ref, o_s.at[rel], o_r.at[rel], dev(chip, other))

    for j, hd in heads():
        @pl.when(hd == px)
        def _():
            q_side(j).wait_send()

        @pl.when(hd != px)
        def _():
            kv_send(j, hd).wait_send()
            for k in range(2):
                q_send(j, hd, k).wait_send()
    for rel in (2, 1, 3, 0):
        b = (px + rel) % side
        val = output_rows(b // 2, q_cols_of(b))
        if rel:
            qst[rel // 2, rel % 2] = val
            o_send(rel).start()
        else:
            og[px] = val
    wo_copy(last).wait()
    wide = d_model // 3
    for rel in (0, 1, 3, 2):
        if rel:
            o_in(rel).wait_recv()
        head = (px - rel + side) % side
        rows = pl.ds(pl.multiple_of(head * head_dim, head_dim), head_dim)
        for j in range(3):
            cols = pl.ds(j * wide, wide)
            prod = jnp.dot(og[head], wob[slot, rows, cols], preferred_element_type=F32)
            if rel == 0:
                part[:, cols] = prod
            elif rel != 2:
                part[:, cols] = part[:, cols] + prod
            else:
                out[:, cols] = (xb[:, cols].astype(F32) + (part[:, cols] + prod)).astype(BF16)
    d_own.wait_send()
    for rel in range(1, side):
        o_send(rel).wait_send()

    @pl.when(main)
    def _():
        for dx in range(side):
            for kind in range(4):
                y_copy(dx, kind).wait_send()
            for dy in range(side):
                to_side(dx, dy).wait_send()


def solution(mesh):
    n_cp = mesh.shape["cp"]

    def device_body(hidden, w_query, w_key, w_value, w_out):
        n_tok, d_model = hidden.shape
        n_layers, n_heads, head_dim, _ = w_out.shape
        half_w = n_heads // 2 * head_dim
        n_loc = n_layers - 1
        n_t2 = n_tok - N_T1
        flat = n_heads * head_dim // LANES * d_model
        n_copy = (4 * N_T1 + 5 * n_t2) // PIECE + 2
        vmem = pl.BlockSpec(memory_space=pltpu.VMEM)
        hbm = pl.BlockSpec(memory_space=pl.ANY)
        scratch = [
            pltpu.VMEM((n_tok, d_model), BF16),
            pltpu.VMEM((2 * n_tok, d_model), BF16),
            pltpu.VMEM((n_loc, 4 * n_tok, d_model), BF16),
            pltpu.VMEM((4 * n_tok, LANES), jnp.int32),
            pltpu.VMEM((n_loc, n_t2, d_model), BF16),
            pltpu.VMEM((n_cp // 2, 2, 2 * n_tok, head_dim), BF16),
            pltpu.VMEM((n_heads // 2, 2, 2 * n_tok, head_dim), BF16),
            pltpu.VMEM((n_heads // 2, 2, head_dim, n_tok), BF16),
            pltpu.VMEM((n_heads, head_dim, n_tok), BF16),
            pltpu.VMEM((n_heads, n_tok, head_dim), BF16),
            pltpu.VMEM((3, flat, LANES), BF16),
            pltpu.VMEM((n_heads * head_dim, LANES), F32),
            pltpu.VMEM((2, 3, d_model, half_w), BF16),
            pltpu.VMEM((2, n_heads * head_dim, d_model), BF16),
            pltpu.VMEM((half_w, 2 * n_tok), BF16),
            pltpu.VMEM((6 * n_tok, half_w), BF16),
            pltpu.VMEM((6 * n_tok, half_w), BF16),
            pltpu.VMEM((n_heads // 2, head_dim, 2 * n_tok), F32),
            pltpu.VMEM((n_heads // 2, 8, 2 * n_tok), F32),
            pltpu.VMEM((n_heads // 2, 8, 2 * n_tok), F32),
            pltpu.VMEM((2, n_tok, half_w), BF16),
            pltpu.VMEM((n_tok, half_w), BF16),
            pltpu.VMEM((n_tok, d_model), F32),
            pltpu.SemaphoreType.DMA((3,)),
            pltpu.SemaphoreType.DMA((2,)),
            pltpu.SemaphoreType.DMA((n_layers, n_copy)),
            pltpu.SemaphoreType.DMA((n_layers, n_copy)),
            pltpu.SemaphoreType.DMA((n_heads // 2 * 4,)),
            pltpu.SemaphoreType.DMA((n_heads,)),
            pltpu.SemaphoreType.DMA((n_heads,)),
            pltpu.SemaphoreType.DMA((n_cp // 2,)),
            pltpu.SemaphoreType.DMA((n_cp // 2,)),
            pltpu.SemaphoreType.DMA((n_cp // 2,)),
            pltpu.SemaphoreType.DMA((n_cp // 2,)),
            pltpu.SemaphoreType.DMA((n_heads,)),
            pltpu.SemaphoreType.DMA((n_heads,)),
        ]
        return pl.pallas_call(
            functools.partial(kernel, n_cp, n_layers, n_heads, head_dim),
            out_shape=jax.ShapeDtypeStruct(hidden.shape, hidden.dtype),
            in_specs=[vmem, hbm, hbm, hbm, hbm],
            out_specs=vmem,
            scratch_shapes=scratch,
            compiler_params=pltpu.CompilerParams(collective_id=0, has_side_effects=True, vmem_limit_bytes=66_500_000),
        )(hidden, flat_view(w_query), flat_view(w_key), flat_view(w_value),
          w_out.reshape(n_layers, n_heads * head_dim, d_model))

    row_spec = P(("dp", "cp"), None)
    return jax.shard_map(device_body, mesh=mesh, in_specs=(row_spec, P(), P(), P(), P()), out_specs=row_spec, check_vma=False)
```

```python
import functools
import math

import jax
import jax.numpy as jnp
from jax import lax
from jax.experimental import pallas as pl
from jax.experimental.pallas import tpu as pltpu
from jax.sharding import PartitionSpec as P

WINDOW = 1024
NORM_EPS = 1e-6
NEG_BIG = -1e30
BF16 = jnp.bfloat16
F32 = jnp.float32
LANES = 128
N_T1 = 160
PIECE = 32
N_1 = N_T1 // PIECE

BLOCKS = ((0, 1), (0, 3), (1, 1), (1, 3), (0, 2), (3, 1), (3, 3), (2, 1), (2, 3), (1, 2), (3, 2), (2, 2))
ARRIVE_AT = {("y", 1): 0, ("opp", 0): 3, ("y", 3): 4, ("y", 2): 6, ("opp", 1): 8, ("opp", 3): 9, ("opp", 2): 10}


def flat_view(weight):
    n_layers, d_model, n_heads, head_dim = weight.shape
    split = weight.reshape(n_layers, d_model, n_heads, head_dim // LANES, LANES)
    return split.transpose(0, 1, 3, 2, 4).reshape(n_layers, -1, LANES)


def table(index, values):
    out = jnp.int32(values[0])
    for pos, value in enumerate(values):
        if pos and value != values[0]:
            out = jnp.where(index == pos, jnp.int32(value), out)
    return out


def kernel(n_cp, n_layers, n_heads, head_dim, x_in, wq, wk, wv, wo, out,
           xb, hown, hh, tk, relay, kvg, st, qst, qg, og, raw, fs, wc, wob, qt, kb, vb,
           acc, m_st, l_st, obuf, osend, part,
           raw_sem, wo_sem, ls, lr, st_s, kv_s, kv_r, q_r, ys, yr, ds, dr, o_s, o_r):
    n_tok, d_model = x_in.shape
    n_chip = n_cp // 2
    side = math.isqrt(n_chip)
    half_w = n_heads // 2 * head_dim
    n_ct = head_dim // LANES
    n_t2 = n_tok - N_T1
    scale = head_dim ** -0.5
    me = lax.axis_index("cp")
    chip = me // 2
    core = me % 2
    other = 1 - core
    px, py = chip % side, chip // side

    def at_xy(x, y):
        return ((y + side) % side) * side + (x + side) % side

    def ring(step):
        return (chip + n_chip + step) % n_chip

    def dev(c, k=None):
        return {"cp": c * 2 + (core if k is None else k)}

    nxt, prv = ring(1), ring(-1)
    xm, xp = at_xy(px - 1, py), at_xy(px + 1, py)
    ym, yp = at_xy(px, py - 1), at_xy(px, py + 1)

    def pass_to(c):
        x, y = c % side, c // side
        return at_xy(x - 1, y + jnp.where(x == 2, 1, 0))

    via = pass_to(chip)
    via_from = at_xy(px + 1, py - jnp.where(px == 1, 1, 0))
    skip_to = (via_from + 2) % n_chip
    skip_from = pass_to(ring(-2))

    barrier = pltpu.get_barrier_semaphore()
    peers = [dev(c) for c in (nxt, prv, ym, yp, via, via_from, skip_to, skip_from)] + [dev(chip, other)]
    peers += [dev(at_xy(px + d, py), k) for d in range(1, side) for k in range(2)]
    for peer in peers:
        pl.semaphore_signal(barrier, inc=1, device_id=peer, device_id_type=pl.DeviceIdType.MESH)

    def raw_copy(layer, i):
        return pltpu.make_async_copy((wq, wk, wv)[i].at[layer], raw.at[i], raw_sem.at[i])

    def wo_copy(layer):
        slot = layer % 2
        return pltpu.make_async_copy(wo.at[layer], wob.at[slot], wo_sem.at[slot])

    for i in range(3):
        raw_copy(0, i).start()
    wo_copy(0).start()
    xb[...] = x_in[...]

    def convert(layer, which=(0, 1, 2)):
        slot = layer % 2
        d_step = fs.shape[0] // (n_heads * n_ct)
        for i in which:
            raw_copy(layer, i).wait()

            def chunk(j, carry):
                r0 = pl.multiple_of(j * fs.shape[0], fs.shape[0])
                d0 = pl.multiple_of(j * d_step, d_step)
                fs[...] = raw[i, pl.ds(r0, fs.shape[0]), :].astype(F32)
                for hd in range(n_heads // 2):
                    for ct in range(n_ct):
                        first = ct * n_heads + core * (n_heads // 2) + hd
                        piece = fs[pl.ds(first, d_step, stride=n_heads * n_ct), :]
                        wc[slot, i, pl.ds(d0, d_step), pl.ds(hd * head_dim + ct * LANES, LANES)] = piece.astype(BF16)
                return carry
            lax.fori_loop(0, d_model // d_step, chunk, 0)

    def project(rows, slot, which, dst):
        for j in range(half_w // head_dim):
            cols = pl.ds(j * head_dim, head_dim)
            dst[:, cols] = jnp.dot(rows, wc[slot, which, :, cols], preferred_element_type=F32).astype(BF16)

    def project_q(rows, slot, q_cols):
        for j in range(half_w // head_dim):
            cols = pl.ds(j * head_dim, head_dim)
            val = jnp.dot(rows, wc[slot, 0, :, cols], preferred_element_type=F32).astype(BF16)
            qt[cols, q_cols] = (val * BF16(scale)).T

    def soft_step(k_val, q_val, v_val, hd, q_cols, mask=None, first=False):
        s = jnp.dot(k_val, q_val, preferred_element_type=F32)
        if mask is not None:
            s = jnp.where(mask, s, NEG_BIG)
        new_m = jnp.max(s, axis=0, keepdims=True)
        if not first:
            old_m = m_st[hd, :1, q_cols]
            new_m = jnp.maximum(old_m, new_m)
        p = jnp.exp(s - new_m)
        part_sum = jnp.sum(p.reshape(p.shape[0] // 8, 8, p.shape[1]), axis=0)
        pv = lax.dot_general(v_val, p.astype(BF16), (((0,), (0,)), ((), ())), preferred_element_type=F32)
        if first:
            l_st[hd, :, q_cols] = part_sum
            acc[hd, :, q_cols] = pv
        else:
            alpha = jnp.exp(old_m - new_m)
            l_st[hd, :, q_cols] = l_st[hd, :, q_cols] * alpha + part_sum
            acc[hd, :, q_cols] = acc[hd, :, q_cols] * alpha + pv
        m_st[hd, :1, q_cols] = new_m

    def update(qi, hd, k_ref, v_ref, mask=None, first=False):
        dims = pl.ds(hd * head_dim, head_dim)
        q_cols = pl.ds(qi * n_tok if isinstance(qi, int) else pl.multiple_of(qi * n_tok, n_tok), n_tok)
        soft_step(k_ref[:, dims], qt[dims, q_cols], v_ref[:, dims], hd, q_cols, mask, first)

    def update_all(k_ref, v_ref, mask_of=None, which=(0, 1)):
        for qi in which:
            mask = None if mask_of is None else mask_of(qi)
            for hd in range(n_heads // 2):
                update(qi, hd, k_ref, v_ref, mask)

    def output_rows(hd, q_cols):
        total = jnp.sum(l_st[hd, :, q_cols], axis=0, keepdims=True)
        return (acc[hd, :, q_cols] / total).astype(BF16).T

    def normed(lo=0, n=n_tok):
        xf = xb[lo:lo + n, :].astype(F32)
        return (xf * lax.rsqrt(jnp.mean(xf * xf, axis=-1, keepdims=True) + NORM_EPS)).astype(BF16)

    def o_copy(layer):
        return pltpu.make_async_remote_copy(osend, obuf.at[core], ls.at[layer, ls.shape[1] - 1], lr.at[layer, lr.shape[1] - 1],
                                            device_id=dev(chip, other), device_id_type=pl.DeviceIdType.MESH)

    def out_own(layer):
        slot = layer % 2
        wo_copy(layer).wait()
        wide = d_model // 3
        mine = pl.ds(pl.multiple_of(core * half_w, half_w), half_w)
        for j in range(3):
            cols = pl.ds(j * wide, wide)
            part[:, cols] = jnp.dot(obuf[core], wob[slot, mine, cols], preferred_element_type=F32)

    def out_other(layer, lo, n):
        slot = layer % 2
        wide = d_model // 3
        theirs = pl.ds(pl.multiple_of(other * half_w, half_w), half_w)
        for j in range(3):
            cols = pl.ds(j * wide, wide)
            prod = part[lo:lo + n, cols] + jnp.dot(obuf[other, lo:lo + n, :], wob[slot, theirs, cols], preferred_element_type=F32)
            xb[lo:lo + n, cols] = (xb[lo:lo + n, cols].astype(F32) + prod).astype(BF16)

    def ici(layer, i, src, dst, c, k=None):
        return pltpu.make_async_remote_copy(src, dst, ls.at[layer, i], lr.at[layer, i],
                                            device_id=dev(c, k), device_id_type=pl.DeviceIdType.MESH)

    n_2 = n_t2 // PIECE
    both = 2 * PIECE
    off_near1 = [ch * both for ch in range(N_1)]
    off_far2 = [2 * N_T1 + ch * both for ch in range(n_2)]
    off_near2, off_far1, groups = [], [], []
    at_row = 2 * n_tok
    per = -(-N_1 // n_2)
    for ch in range(n_2):
        first = at_row
        off_near2.append(at_row)
        at_row += both
        far_ids = list(range(ch * per, min(N_1, (ch + 1) * per)))
        for _ in far_ids:
            off_far1.append(at_row)
            at_row += both
        groups.append((first, at_row - first, far_ids))
    key_i = lax.broadcasted_iota(jnp.int32, tk.shape, 0)
    limit = jnp.full(tk.shape, 4 * n_tok, jnp.int32)
    for offs, base in ((off_far1, 0), (off_far2, N_T1)):
        for ch, off in enumerate(offs):
            for k in range(2):
                start = off + k * PIECE
                inside = (key_i >= start) & (key_i < start + PIECE)
                shift = k * n_tok + base + ch * PIECE + WINDOW - 4 * n_tok - start
                limit = jnp.where(inside, jnp.where(chip >= 2, key_i + shift, -1), limit)
    tk[...] = limit

    mine = pl.ds(pl.multiple_of(core * n_tok, n_tok), n_tok)

    def own_rows(lo, n):
        return hown.at[pl.ds(pl.multiple_of(core * n_tok + lo, 16), n), :]

    def own_copies(layer):
        hl = hh.at[layer]
        t1 = [ici(layer, ch, own_rows(ch * PIECE, PIECE), hl.at[piece_rows(off), :], nxt) for ch, off in enumerate(off_near1)]
        t2 = [ici(layer, N_1 + ch, own_rows(N_T1 + ch * PIECE, PIECE), relay.at[layer, pl.ds(ch * PIECE, PIECE), :], via)
              for ch in range(n_2)]
        side_own = ici(layer, N_1 + n_2, hown.at[mine], hown.at[mine], chip, other)
        return t1, t2, side_own

    def piece_rows(off):
        return pl.ds(pl.multiple_of(off + core * PIECE, 16), PIECE)

    def launch1():
        hown[pl.ds(pl.multiple_of(core * n_tok, n_tok), N_T1), :] = normed(0, N_T1)

    def launch2():
        hown[pl.ds(pl.multiple_of(core * n_tok + N_T1, 16), n_t2), :] = normed(N_T1, n_t2)

    def local_layer(layer, carry):
        slot = layer % 2
        t1_own, t2_own, d_own = own_copies(layer)
        base = N_1 + n_2 + 1

        def piece(off):
            return hh.at[layer, piece_rows(off), :]

        near1, far1 = [piece(off) for off in off_near1], [piece(off) for off in off_far1]
        near2, far2 = [piece(off) for off in off_near2], [piece(off) for off in off_far2]
        pass2 = [relay.at[layer, pl.ds(ch * PIECE, PIECE), :] for ch in range(n_2)]

        def series(srcs, dsts, c, k=None):
            nonlocal base
            out = [ici(layer, base + i, a, b, c, k) for i, (a, b) in enumerate(zip(srcs, dsts))]
            base += len(out)
            return out

        t1_fwd = series(near1, far1, nxt)
        t2_relay = series(pass2, far2, skip_to)
        t2_fwd = series(far2, near2, prv)
        d_n1 = series(near1, near1, chip, other)
        d_f1 = series(far1, far1, chip, other)
        d_n2 = series(near2, near2, chip, other)
        d_f2 = series(far2, far2, chip, other)
        oc = o_copy(layer)

        @pl.when(layer == 0)
        def _():
            launch1()
            pl.semaphore_wait(barrier, len(peers))
            for cp in t1_own:
                cp.start()
            launch2()
            for cp in t2_own:
                cp.start()
            d_own.start()
        wo_copy(layer + 1).start()

        def own_block(b):
            dst_rows = pl.ds(pl.multiple_of(b * n_tok, n_tok), n_tok)
            rows = hown[dst_rows, :]
            project_q(rows, slot, dst_rows)
            project(rows, slot, 1, kb.at[dst_rows])
            project(rows, slot, 2, vb.at[dst_rows])

        def take(arrived, onward, side_copy):
            arrived.wait_recv()
            if onward is not None:
                onward.start()
            if side_copy is not None:
                side_copy.start()

        def take_n1(ch):
            take(t1_own[ch], t1_fwd[ch], d_n1[ch])

        def take_pass(ch):
            take(t2_own[ch], t2_relay[ch], None)

        def take_f2(ch):
            take(t2_relay[ch], t2_fwd[ch], d_f2[ch])

        def take_late(g):
            for ch in groups[g][2]:
                take(t1_fwd[ch], None, d_f1[ch])
            take(t2_fwd[g], None, d_n2[g])

        def side_late(g):
            for ch in groups[g][2]:
                d_f1[ch].wait_recv()
            d_n2[g].wait_recv()

        def kv_rows(lo, n):
            @pl.when(chip >= 1)
            def _():
                rows = hh[layer, lo:lo + n]
                project(rows, slot, 1, kb.at[pl.ds(2 * n_tok + lo, n)])
                project(rows, slot, 2, vb.at[pl.ds(2 * n_tok + lo, n)])

        lane_i = lax.broadcasted_iota(jnp.int32, (1, n_tok), 1)

        def attend(lo, n, which=(0, 1)):
            def mask_of(qi):
                rows = tk[lo:lo + n, :]
                return jnp.concatenate([rows] * (n_tok // LANES), axis=1) > lane_i + qi * n_tok

            @pl.when(chip >= 1)
            def _():
                at = pl.ds(2 * n_tok + lo, n)
                update_all(kb.at[at], vb.at[at], mask_of, which)

        @pl.when(layer == 0)
        def _():
            for ch in range(3):
                convert(0, (ch,))
                take_pass(ch)
                take_n1(ch)
            for i in range(3):
                raw_copy(1, i).start()

        own_block(core)
        d_own.wait_recv()
        own_block(other)
        row_i = lax.broadcasted_iota(jnp.int32, (2 * n_tok, n_tok), 0)
        col_i = lax.broadcasted_iota(jnp.int32, (2 * n_tok, n_tok), 1)
        for hd in range(n_heads // 2):
            update(0, hd, kb.at[:n_tok], vb.at[:n_tok], row_i[:n_tok] <= col_i[:n_tok], first=True)
            update(1, hd, kb.at[:2 * n_tok], vb.at[:2 * n_tok], row_i <= col_i + n_tok, first=True)
        for ch in range(3):
            @pl.when(layer > 0)
            def _():
                take_pass(ch)
                take_n1(ch)
            if ch == 2:
                take_n1(3)
                take_f2(0)
            convert(layer + 1, (ch,))

        @pl.when(layer + 2 < n_layers)
        def _():
            for i in range(3):
                raw_copy(layer + 2, i).start()

        take_n1(4)
        take_f2(1)
        for ch in range(N_1):
            d_n1[ch].wait_recv()
        kv_rows(0, 2 * N_T1)
        take_f2(2)
        for ch in range(n_2):
            d_f2[ch].wait_recv()
        kv_rows(2 * N_T1, 2 * n_t2)
        take_late(0)
        attend(0, 2 * n_tok)
        for g in range(n_2):
            side_late(g)
            if g == n_2 - 2:
                take_late(g + 1)
            kv_rows(*groups[g][:2])
            if g < n_2 - 2:
                take_late(g + 1)
            if g < n_2 - 1:
                attend(*groups[g][:2])

        def put(qi, dst):
            for hd in range(n_heads // 2):
                dst[:, pl.ds(hd * head_dim, head_dim)] = output_rows(hd, pl.ds(pl.multiple_of(qi * n_tok, n_tok), n_tok))

        attend(*groups[n_2 - 1][:2], which=(other,))
        put(other, osend)
        oc.start()
        attend(*groups[n_2 - 1][:2], which=(core,))
        put(core, obuf.at[core])
        out_own(layer)
        for group in (t1_own, t1_fwd, t2_own, t2_relay, t2_fwd, d_n1, d_f1, d_n2, d_f2, [d_own]):
            for cp in group:
                cp.wait_send()
        oc.wait_recv()
        go_on = layer + 1 < n_layers - 1
        later1, later2, later_own = own_copies(layer + 1)
        out_other(layer, 0, N_T1)

        @pl.when(go_on)
        def _():
            launch1()
            for cp in later1:
                cp.start()
        out_other(layer, N_T1, n_t2)

        @pl.when(go_on)
        def _():
            launch2()
            for cp in later2:
                cp.start()
            later_own.start()
        oc.wait_send()
        return carry

    lax.fori_loop(0, n_layers - 1, local_layer, 0)

    last = n_layers - 1
    slot = last % 2
    per_core = n_heads // 2
    main = core == px // per_core
    launch1()
    launch2()
    d_own = ici(last, 0, hown.at[mine], hown.at[mine], chip, other)
    d_own.start()
    m_st[...] = jnp.full(m_st.shape, NEG_BIG, F32)
    l_st[...] = jnp.zeros(l_st.shape, F32)
    acc[...] = jnp.zeros(acc.shape, F32)

    def rcopy(src, dst, send_sem, recv_sem, target):
        return pltpu.make_async_remote_copy(src, dst, send_sem, recv_sem, device_id=target, device_id_type=pl.DeviceIdType.MESH)

    def rel_to(hd):
        return (px - hd + side) % side

    def heads():
        return [(j, core * per_core + j) for j in range(per_core)]

    def half_rows(b):
        return pl.ds(pl.multiple_of(b * n_tok, n_tok), n_tok)

    def kv_send(j, hd, b):
        rel = rel_to(hd)
        return rcopy(st.at[j, :, half_rows(b)], kvg.at[chip, :, half_rows(b)], kv_s.at[j * 2 + b], kv_r.at[rel * 2 + b], dev(at_xy(hd, py)))

    def own_y(way, b):
        ref = kvg.at[chip, :, half_rows(b)]
        return rcopy(ref, ref, kv_s.at[2 * per_core + way * 2 + b], kv_r.at[2 * n_heads + way * 2 + b], dev(yp if way == 0 else ym))

    def half_in(c, i, b):
        ref = kvg.at[c, :, half_rows(b)]
        return rcopy(ref, ref, kv_s.at[0], kv_r.at[i * 2 + b], dev(chip, other))

    def q_send(j, hd, k):
        i = per_core + 2 * j + k
        return rcopy(qst.at[j, k], qg.at[px], st_s.at[i], q_r.at[rel_to(hd)], dev(at_xy(hd, py), k))

    def q_side(j):
        i = per_core + 2 * per_core + j
        return rcopy(qst.at[j, other], qg.at[px], st_s.at[i], q_r.at[0], dev(chip, other))

    def block_chip(dx, dy):
        return at_xy(px + dx, py + dy)

    def y_copy(dx, kind):
        if kind < 2:
            ref = kvg.at[block_chip(dx, 0)]
        else:
            ref = kvg.at[block_chip(dx, -1 if kind == 2 else 1), kind - 2]
        i = dx * 4 + kind
        return rcopy(ref, ref, ys.at[i], yr.at[i], dev(yp if kind % 2 == 0 else ym))

    def to_side(dx, dy):
        ref = kvg.at[block_chip(dx, dy)]
        i = dx * side + dy
        return rcopy(ref, ref, ds.at[i], dr.at[i], dev(chip, other))

    def own_kv(b):
        seg = pl.ds(pl.multiple_of(b * n_tok, n_tok), n_tok)
        rows = hown[seg, :]
        for j in range(per_core):
            cols = pl.ds(j * head_dim, head_dim)
            for i in range(2):
                st[j, i, seg, :] = jnp.dot(rows, wc[slot, 1 + i, :, cols], preferred_element_type=F32).astype(BF16)

    def own_q(b):
        rows = hown[pl.ds(pl.multiple_of(b * n_tok, n_tok), n_tok), :]
        for j in range(per_core):
            cols = pl.ds(j * head_dim, head_dim)
            val = jnp.dot(rows, wc[slot, 0, :, cols], preferred_element_type=F32).astype(BF16)
            qst[j, b] = (val * BF16(scale)).T

    def send_half(b):
        for j, hd in heads():
            @pl.when(hd == px)
            def _():
                kvg[chip, :, half_rows(b)] = st[j, :, half_rows(b)]
                for way in range(2):
                    own_y(way, b).start()

            @pl.when((hd != px) & (rel_to(hd) != 2))
            def _():
                kv_send(j, hd, b).start()

    own_kv(core)
    send_half(core)
    d_own.wait_recv()
    own_kv(other)
    send_half(other)

    @pl.when(main)
    def _():
        to_side(0, 0).start()
    own_q(core)
    own_q(other)
    for j, hd in heads():
        @pl.when(rel_to(hd) == 2)
        def _():
            for b in range(2):
                kv_send(j, hd, b).start()
    for j, hd in heads():
        @pl.when(hd == px)
        def _():
            q_side(j).start()
            qg[px] = qst[j, core]

        @pl.when(hd != px)
        def _():
            for k in range(2):
                q_send(j, hd, k).start()

    def arrive(what, dx):
        @pl.when(main)
        def _():
            if what == "row":
                for b in range(2):
                    half_in(block_chip(dx, 0), dx, b).wait_recv()
                y_copy(dx, 0).start()
                y_copy(dx, 1).start()
                to_side(dx, 0).start()
            elif what == "y":
                for kind in range(2):
                    if dx:
                        y_copy(dx, kind).wait_recv()
                    else:
                        for b in range(2):
                            half_in(block_chip(0, -1 if kind == 0 else 1), n_heads + kind, b).wait_recv()
                for kind in range(2, 4):
                    y_copy(dx, kind).start()
                to_side(dx, side - 1).start()
                to_side(dx, 1).start()
            else:
                for kind in range(2, 4):
                    rcopy(kvg.at[block_chip(dx, 2), kind - 2], kvg.at[block_chip(dx, 2), kind - 2], ys.at[dx * 4 + kind],
                          yr.at[dx * 4 + kind], dev(chip, other)).wait_recv()
                to_side(dx, 2).start()

    def have(dx, dy, i):
        @pl.when(jnp.logical_not(main))
        def _():
            c = block_chip(dx, dy)
            rcopy(kvg.at[c], kvg.at[c], ds.at[i], dr.at[i], dev(chip, other)).wait_recv()

    arrive("row", 1)
    arrive("row", side - 1)
    arrive("y", 0)
    arrive("row", 2)
    for dx in range(side):
        q_in = rcopy(qst.at[0, 0], qg.at[(px + dx) % side], st_s.at[0], q_r.at[dx], dev(chip, other))
        if dx == 0:
            @pl.when(jnp.logical_not(main))
            def _():
                q_in.wait_recv()
        else:
            q_in.wait_recv()

    def q_cols_of(b):
        return pl.ds(pl.multiple_of(b % 2 * n_tok, n_tok), n_tok)

    key_i = lax.broadcasted_iota(jnp.int32, (2 * n_tok, n_tok), 0)
    query_i = lax.broadcasted_iota(jnp.int32, (2 * n_tok, n_tok), 1) + core * n_tok

    def row_step(dx, carry):
        src_x = (px + dx) % side
        have(dx, 0, dx * side)
        c = block_chip(dx, 0)

        def one(b, c2):
            @pl.when(src_x <= b)
            def _():
                mask = key_i - query_i <= (b - src_x) * (2 * n_tok)
                soft_step(kvg[c, 0], qg[b], kvg[c, 1], b // 2, q_cols_of(b), mask)
            return c2

        lax.fori_loop(0, side, one, 0)
        return carry

    lax.fori_loop(0, side, row_step, 0)

    def block_step(i, carry):
        for (what, col), when in ARRIVE_AT.items():
            @pl.when(i == when)
            def _():
                arrive(what, col)
        dx = table(i, [blk[0] for blk in BLOCKS])
        dy = table(i, [blk[1] for blk in BLOCKS])
        have(dx, dy, dx * side + dy)
        c = block_chip(dx, dy)

        @pl.when(c // side < py)
        def _():
            for b in range(side):
                soft_step(kvg[c, 0], qg[b], kvg[c, 1], b // 2, pl.ds(b % 2 * n_tok, n_tok))
        return carry

    lax.fori_loop(0, len(BLOCKS), block_step, 0)

    def o_send(rel):
        b = (px + rel) % side
        return rcopy(qst.at[rel // 2, rel % 2], og.at[px], o_s.at[rel], o_r.at[rel], dev(at_xy(px + rel, py)))

    def o_in(rel):
        ref = og.at[(px - rel + side) % side]
        return rcopy(ref, ref, o_s.at[rel], o_r.at[rel], dev(chip, other))

    for j, hd in heads():
        @pl.when(hd == px)
        def _():
            q_side(j).wait_send()

        @pl.when(hd != px)
        def _():
            for k in range(2):
                kv_send(j, hd, k).wait_send()
                q_send(j, hd, k).wait_send()
    for rel in (2, 1, 3, 0):
        b = (px + rel) % side
        val = output_rows(b // 2, q_cols_of(b))
        if rel:
            qst[rel // 2, rel % 2] = val
            o_send(rel).start()
        else:
            og[px] = val
    wo_copy(last).wait()
    wide = d_model // 3
    for rel in (0, 1, 3, 2):
        if rel:
            o_in(rel).wait_recv()
        head = (px - rel + side) % side
        rows = pl.ds(pl.multiple_of(head * head_dim, head_dim), head_dim)
        for j in range(3):
            cols = pl.ds(j * wide, wide)
            prod = jnp.dot(og[head], wob[slot, rows, cols], preferred_element_type=F32)
            if rel == 0:
                part[:, cols] = prod
            elif rel != 2:
                part[:, cols] = part[:, cols] + prod
            else:
                out[:, cols] = (xb[:, cols].astype(F32) + (part[:, cols] + prod)).astype(BF16)
    d_own.wait_send()
    for rel in range(1, side):
        o_send(rel).wait_send()

    @pl.when(main)
    def _():
        for way in range(2):
            for b in range(2):
                own_y(way, b).wait_send()
        for dx in range(side):
            for kind in range(0 if dx else 2, 4):
                y_copy(dx, kind).wait_send()
            for dy in range(side):
                to_side(dx, dy).wait_send()


def solution(mesh):
    n_cp = mesh.shape["cp"]

    def device_body(hidden, w_query, w_key, w_value, w_out):
        n_tok, d_model = hidden.shape
        n_layers, n_heads, head_dim, _ = w_out.shape
        half_w = n_heads // 2 * head_dim
        n_loc = n_layers - 1
        n_t2 = n_tok - N_T1
        flat = n_heads * head_dim // LANES * d_model
        n_copy = (4 * N_T1 + 5 * n_t2) // PIECE + 2
        vmem = pl.BlockSpec(memory_space=pltpu.VMEM)
        hbm = pl.BlockSpec(memory_space=pl.ANY)
        scratch = [
            pltpu.VMEM((n_tok, d_model), BF16),
            pltpu.VMEM((2 * n_tok, d_model), BF16),
            pltpu.VMEM((n_loc, 4 * n_tok, d_model), BF16),
            pltpu.VMEM((4 * n_tok, LANES), jnp.int32),
            pltpu.VMEM((n_loc, n_t2, d_model), BF16),
            pltpu.VMEM((n_cp // 2, 2, 2 * n_tok, head_dim), BF16),
            pltpu.VMEM((n_heads // 2, 2, 2 * n_tok, head_dim), BF16),
            pltpu.VMEM((n_heads // 2, 2, head_dim, n_tok), BF16),
            pltpu.VMEM((n_heads, head_dim, n_tok), BF16),
            pltpu.VMEM((n_heads, n_tok, head_dim), BF16),
            pltpu.VMEM((3, flat, LANES), BF16),
            pltpu.VMEM((n_heads * head_dim, LANES), F32),
            pltpu.VMEM((2, 3, d_model, half_w), BF16),
            pltpu.VMEM((2, n_heads * head_dim, d_model), BF16),
            pltpu.VMEM((half_w, 2 * n_tok), BF16),
            pltpu.VMEM((6 * n_tok, half_w), BF16),
            pltpu.VMEM((6 * n_tok, half_w), BF16),
            pltpu.VMEM((n_heads // 2, head_dim, 2 * n_tok), F32),
            pltpu.VMEM((n_heads // 2, 8, 2 * n_tok), F32),
            pltpu.VMEM((n_heads // 2, 8, 2 * n_tok), F32),
            pltpu.VMEM((2, n_tok, half_w), BF16),
            pltpu.VMEM((n_tok, half_w), BF16),
            pltpu.VMEM((n_tok, d_model), F32),
            pltpu.SemaphoreType.DMA((3,)),
            pltpu.SemaphoreType.DMA((2,)),
            pltpu.SemaphoreType.DMA((n_layers, n_copy)),
            pltpu.SemaphoreType.DMA((n_layers, n_copy)),
            pltpu.SemaphoreType.DMA((n_heads // 2 * 4,)),
            pltpu.SemaphoreType.DMA((n_heads + 4,)),
            pltpu.SemaphoreType.DMA((2 * n_heads + 4,)),
            pltpu.SemaphoreType.DMA((n_heads,)),
            pltpu.SemaphoreType.DMA((n_cp // 2,)),
            pltpu.SemaphoreType.DMA((n_cp // 2,)),
            pltpu.SemaphoreType.DMA((n_cp // 2,)),
            pltpu.SemaphoreType.DMA((n_cp // 2,)),
            pltpu.SemaphoreType.DMA((n_heads,)),
            pltpu.SemaphoreType.DMA((n_heads,)),
        ]
        return pl.pallas_call(
            functools.partial(kernel, n_cp, n_layers, n_heads, head_dim),
            out_shape=jax.ShapeDtypeStruct(hidden.shape, hidden.dtype),
            in_specs=[vmem, hbm, hbm, hbm, hbm],
            out_specs=vmem,
            scratch_shapes=scratch,
            compiler_params=pltpu.CompilerParams(collective_id=0, has_side_effects=True, vmem_limit_bytes=66_500_000),
        )(hidden, flat_view(w_query), flat_view(w_key), flat_view(w_value),
          w_out.reshape(n_layers, n_heads * head_dim, d_model))

    row_spec = P(("dp", "cp"), None)
    return jax.shard_map(device_body, mesh=mesh, in_specs=(row_spec, P(), P(), P(), P()), out_specs=row_spec, check_vma=False)
```

```python
import functools
import math

import jax
import jax.numpy as jnp
from jax import lax
from jax.experimental import pallas as pl
from jax.experimental.pallas import tpu as pltpu
from jax.sharding import PartitionSpec as P

WINDOW = 1024
NORM_EPS = 1e-6
NEG_BIG = -1e30
BF16 = jnp.bfloat16
F32 = jnp.float32
LANES = 128
N_T1 = 160
PIECE = 32
N_1 = N_T1 // PIECE

BLOCKS = ((0, 1), (0, 3), (1, 1), (1, 3), (0, 2), (3, 1), (3, 3), (2, 1), (2, 3), (1, 2), (3, 2), (2, 2))
ARRIVE_AT = {("y", 1): 0, ("opp", 0): 3, ("y", 3): 4, ("y", 2): 6, ("opp", 1): 8, ("opp", 3): 9, ("opp", 2): 10}


def flat_view(weight):
    n_layers, d_model, n_heads, head_dim = weight.shape
    split = weight.reshape(n_layers, d_model, n_heads, head_dim // LANES, LANES)
    return split.transpose(0, 1, 3, 2, 4).reshape(n_layers, -1, LANES)


def table(index, values):
    out = jnp.int32(values[0])
    for pos, value in enumerate(values):
        if pos and value != values[0]:
            out = jnp.where(index == pos, jnp.int32(value), out)
    return out


def kernel(n_cp, n_layers, n_heads, head_dim, x_in, wq, wk, wv, wo, out,
           xb, hown, hh, tk, relay, kvg, st, qst, qg, og, raw, fs, wc, wob, qt, kb, vb,
           acc, m_st, l_st, obuf, osend, part,
           raw_sem, wo_sem, ls, lr, st_s, kv_s, kv_r, q_r, ys, yr, ds, dr, o_s, o_r):
    n_tok, d_model = x_in.shape
    n_chip = n_cp // 2
    side = math.isqrt(n_chip)
    half_w = n_heads // 2 * head_dim
    n_ct = head_dim // LANES
    n_t2 = n_tok - N_T1
    scale = head_dim ** -0.5
    me = lax.axis_index("cp")
    chip = me // 2
    core = me % 2
    other = 1 - core
    px, py = chip % side, chip // side

    def at_xy(x, y):
        return ((y + side) % side) * side + (x + side) % side

    def ring(step):
        return (chip + n_chip + step) % n_chip

    def dev(c, k=None):
        return {"cp": c * 2 + (core if k is None else k)}

    nxt, prv = ring(1), ring(-1)
    xm, xp = at_xy(px - 1, py), at_xy(px + 1, py)
    ym, yp = at_xy(px, py - 1), at_xy(px, py + 1)

    def pass_to(c):
        x, y = c % side, c // side
        return at_xy(x - 1, y + jnp.where(x == 2, 1, 0))

    via = pass_to(chip)
    via_from = at_xy(px + 1, py - jnp.where(px == 1, 1, 0))
    skip_to = (via_from + 2) % n_chip
    skip_from = pass_to(ring(-2))

    barrier = pltpu.get_barrier_semaphore()
    peers = [dev(c) for c in (nxt, prv, ym, yp, via, via_from, skip_to, skip_from)] + [dev(chip, other)]
    peers += [dev(at_xy(px + d, py), k) for d in range(1, side) for k in range(2)]
    for peer in peers:
        pl.semaphore_signal(barrier, inc=1, device_id=peer, device_id_type=pl.DeviceIdType.MESH)

    def raw_copy(layer, i):
        return pltpu.make_async_copy((wq, wk, wv)[i].at[layer], raw.at[i], raw_sem.at[i])

    def wo_copy(layer):
        slot = layer % 2
        return pltpu.make_async_copy(wo.at[layer], wob.at[slot], wo_sem.at[slot])

    x_copy = pltpu.make_async_copy(x_in, xb, raw_sem.at[3])
    x_copy.start()
    for i in range(3):
        raw_copy(0, i).start()
    wo_copy(0).start()

    def convert(layer, which=(0, 1, 2)):
        slot = layer % 2
        d_step = fs.shape[0] // (n_heads * n_ct)
        for i in which:
            raw_copy(layer, i).wait()

            def chunk(j, carry):
                r0 = pl.multiple_of(j * fs.shape[0], fs.shape[0])
                d0 = pl.multiple_of(j * d_step, d_step)
                fs[...] = raw[i, pl.ds(r0, fs.shape[0]), :].astype(F32)
                for hd in range(n_heads // 2):
                    for ct in range(n_ct):
                        first = ct * n_heads + core * (n_heads // 2) + hd
                        piece = fs[pl.ds(first, d_step, stride=n_heads * n_ct), :]
                        wc[slot, i, pl.ds(d0, d_step), pl.ds(hd * head_dim + ct * LANES, LANES)] = piece.astype(BF16)
                return carry
            lax.fori_loop(0, d_model // d_step, chunk, 0)

    def project(rows, slot, which, dst):
        for j in range(half_w // head_dim):
            cols = pl.ds(j * head_dim, head_dim)
            dst[:, cols] = jnp.dot(rows, wc[slot, which, :, cols], preferred_element_type=F32).astype(BF16)

    def project_q(rows, slot, q_cols):
        for j in range(half_w // head_dim):
            cols = pl.ds(j * head_dim, head_dim)
            val = jnp.dot(rows, wc[slot, 0, :, cols], preferred_element_type=F32).astype(BF16)
            qt[cols, q_cols] = (val * BF16(scale)).T

    def soft_step(k_val, q_val, v_val, hd, q_cols, mask=None, first=False):
        s = jnp.dot(k_val, q_val, preferred_element_type=F32)
        if mask is not None:
            s = jnp.where(mask, s, NEG_BIG)
        new_m = jnp.max(s, axis=0, keepdims=True)
        if not first:
            old_m = m_st[hd, :1, q_cols]
            new_m = jnp.maximum(old_m, new_m)
        p = jnp.exp(s - new_m)
        part_sum = jnp.sum(p.reshape(p.shape[0] // 8, 8, p.shape[1]), axis=0)
        pv = lax.dot_general(v_val, p.astype(BF16), (((0,), (0,)), ((), ())), preferred_element_type=F32)
        if first:
            l_st[hd, :, q_cols] = part_sum
            acc[hd, :, q_cols] = pv
        else:
            alpha = jnp.exp(old_m - new_m)
            l_st[hd, :, q_cols] = l_st[hd, :, q_cols] * alpha + part_sum
            acc[hd, :, q_cols] = acc[hd, :, q_cols] * alpha + pv
        m_st[hd, :1, q_cols] = new_m

    def update(qi, hd, k_ref, v_ref, mask=None, first=False):
        dims = pl.ds(hd * head_dim, head_dim)
        q_cols = pl.ds(qi * n_tok if isinstance(qi, int) else pl.multiple_of(qi * n_tok, n_tok), n_tok)
        soft_step(k_ref[:, dims], qt[dims, q_cols], v_ref[:, dims], hd, q_cols, mask, first)

    def update_all(k_ref, v_ref, mask_of=None, which=(0, 1)):
        for qi in which:
            mask = None if mask_of is None else mask_of(qi)
            for hd in range(n_heads // 2):
                update(qi, hd, k_ref, v_ref, mask)

    def output_rows(hd, q_cols):
        total = jnp.sum(l_st[hd, :, q_cols], axis=0, keepdims=True)
        return (acc[hd, :, q_cols] / total).astype(BF16).T

    def normed(lo=0, n=n_tok):
        xf = xb[lo:lo + n, :].astype(F32)
        return (xf * lax.rsqrt(jnp.mean(xf * xf, axis=-1, keepdims=True) + NORM_EPS)).astype(BF16)

    def o_copy(layer):
        return pltpu.make_async_remote_copy(osend, obuf.at[core], ls.at[layer, ls.shape[1] - 1], lr.at[layer, lr.shape[1] - 1],
                                            device_id=dev(chip, other), device_id_type=pl.DeviceIdType.MESH)

    def out_own(layer):
        slot = layer % 2
        wo_copy(layer).wait()
        wide = d_model // 3
        mine = pl.ds(pl.multiple_of(core * half_w, half_w), half_w)
        for j in range(3):
            cols = pl.ds(j * wide, wide)
            part[:, cols] = jnp.dot(obuf[core], wob[slot, mine, cols], preferred_element_type=F32)

    def out_other(layer, lo, n):
        slot = layer % 2
        wide = d_model // 3
        theirs = pl.ds(pl.multiple_of(other * half_w, half_w), half_w)
        for j in range(3):
            cols = pl.ds(j * wide, wide)
            prod = part[lo:lo + n, cols] + jnp.dot(obuf[other, lo:lo + n, :], wob[slot, theirs, cols], preferred_element_type=F32)
            xb[lo:lo + n, cols] = (xb[lo:lo + n, cols].astype(F32) + prod).astype(BF16)

    def ici(layer, i, src, dst, c, k=None):
        return pltpu.make_async_remote_copy(src, dst, ls.at[layer, i], lr.at[layer, i],
                                            device_id=dev(c, k), device_id_type=pl.DeviceIdType.MESH)

    n_2 = n_t2 // PIECE
    both = 2 * PIECE
    off_near1 = [ch * both for ch in range(N_1)]
    off_far2 = [2 * N_T1 + ch * both for ch in range(n_2)]
    off_near2, off_far1, groups = [], [], []
    at_row = 2 * n_tok
    per = -(-N_1 // n_2)
    for ch in range(n_2):
        first = at_row
        off_near2.append(at_row)
        at_row += both
        far_ids = list(range(ch * per, min(N_1, (ch + 1) * per)))
        for _ in far_ids:
            off_far1.append(at_row)
            at_row += both
        groups.append((first, at_row - first, far_ids))
    key_i = lax.broadcasted_iota(jnp.int32, tk.shape, 0)
    limit = jnp.full(tk.shape, 4 * n_tok, jnp.int32)
    for offs, base in ((off_far1, 0), (off_far2, N_T1)):
        for ch, off in enumerate(offs):
            for k in range(2):
                start = off + k * PIECE
                inside = (key_i >= start) & (key_i < start + PIECE)
                shift = k * n_tok + base + ch * PIECE + WINDOW - 4 * n_tok - start
                limit = jnp.where(inside, jnp.where(chip >= 2, key_i + shift, -1), limit)
    tk[...] = limit

    mine = pl.ds(pl.multiple_of(core * n_tok, n_tok), n_tok)

    def own_rows(lo, n):
        return hown.at[pl.ds(pl.multiple_of(core * n_tok + lo, 16), n), :]

    def own_copies(layer):
        hl = hh.at[layer]
        t1 = [ici(layer, ch, own_rows(ch * PIECE, PIECE), hl.at[piece_rows(off), :], nxt) for ch, off in enumerate(off_near1)]
        t2 = [ici(layer, N_1 + ch, own_rows(N_T1 + ch * PIECE, PIECE), relay.at[layer, pl.ds(ch * PIECE, PIECE), :], via)
              for ch in range(n_2)]
        side_own = ici(layer, N_1 + n_2, hown.at[mine], hown.at[mine], chip, other)
        return t1, t2, side_own

    def piece_rows(off):
        return pl.ds(pl.multiple_of(off + core * PIECE, 16), PIECE)

    def launch1():
        hown[pl.ds(pl.multiple_of(core * n_tok, n_tok), N_T1), :] = normed(0, N_T1)

    def launch2():
        hown[pl.ds(pl.multiple_of(core * n_tok + N_T1, 16), n_t2), :] = normed(N_T1, n_t2)

    def local_layer(layer, carry):
        slot = layer % 2
        t1_own, t2_own, d_own = own_copies(layer)
        base = N_1 + n_2 + 1

        def piece(off):
            return hh.at[layer, piece_rows(off), :]

        near1, far1 = [piece(off) for off in off_near1], [piece(off) for off in off_far1]
        near2, far2 = [piece(off) for off in off_near2], [piece(off) for off in off_far2]
        pass2 = [relay.at[layer, pl.ds(ch * PIECE, PIECE), :] for ch in range(n_2)]

        def series(srcs, dsts, c, k=None):
            nonlocal base
            out = [ici(layer, base + i, a, b, c, k) for i, (a, b) in enumerate(zip(srcs, dsts))]
            base += len(out)
            return out

        t1_fwd = series(near1, far1, nxt)
        t2_relay = series(pass2, far2, skip_to)
        t2_fwd = series(far2, near2, prv)
        d_n1 = series(near1, near1, chip, other)
        d_f1 = series(far1, far1, chip, other)
        d_n2 = series(near2, near2, chip, other)
        d_f2 = series(far2, far2, chip, other)
        oc = o_copy(layer)

        @pl.when(layer == 0)
        def _():
            x_copy.wait()
            launch1()
            pl.semaphore_wait(barrier, len(peers))
            for cp in t1_own:
                cp.start()
            launch2()
            for cp in t2_own:
                cp.start()
            d_own.start()
        wo_copy(layer + 1).start()

        def own_block(b):
            dst_rows = pl.ds(pl.multiple_of(b * n_tok, n_tok), n_tok)
            rows = hown[dst_rows, :]
            project_q(rows, slot, dst_rows)
            project(rows, slot, 1, kb.at[dst_rows])
            project(rows, slot, 2, vb.at[dst_rows])

        def take(arrived, onward, side_copy):
            arrived.wait_recv()
            if onward is not None:
                onward.start()
            if side_copy is not None:
                side_copy.start()

        def take_n1(ch):
            take(t1_own[ch], t1_fwd[ch], d_n1[ch])

        def take_pass(ch):
            take(t2_own[ch], t2_relay[ch], None)

        def take_f2(ch):
            take(t2_relay[ch], t2_fwd[ch], d_f2[ch])

        def take_late(g):
            for ch in groups[g][2]:
                take(t1_fwd[ch], None, d_f1[ch])
            take(t2_fwd[g], None, d_n2[g])

        def side_late(g):
            for ch in groups[g][2]:
                d_f1[ch].wait_recv()
            d_n2[g].wait_recv()

        def kv_rows(lo, n):
            @pl.when(chip >= 1)
            def _():
                rows = hh[layer, lo:lo + n]
                project(rows, slot, 1, kb.at[pl.ds(2 * n_tok + lo, n)])
                project(rows, slot, 2, vb.at[pl.ds(2 * n_tok + lo, n)])

        lane_i = lax.broadcasted_iota(jnp.int32, (1, n_tok), 1)

        def attend(lo, n, which=(0, 1)):
            def mask_of(qi):
                rows = tk[lo:lo + n, :]
                return jnp.concatenate([rows] * (n_tok // LANES), axis=1) > lane_i + qi * n_tok

            @pl.when(chip >= 1)
            def _():
                at = pl.ds(2 * n_tok + lo, n)
                update_all(kb.at[at], vb.at[at], mask_of, which)

        @pl.when(layer == 0)
        def _():
            for ch in range(3):
                convert(0, (ch,))
                take_pass(ch)
                take_n1(ch)
            for i in range(3):
                raw_copy(1, i).start()

        own_block(core)
        d_own.wait_recv()
        own_block(other)
        row_i = lax.broadcasted_iota(jnp.int32, (2 * n_tok, n_tok), 0)
        col_i = lax.broadcasted_iota(jnp.int32, (2 * n_tok, n_tok), 1)
        for hd in range(n_heads // 2):
            update(0, hd, kb.at[:n_tok], vb.at[:n_tok], row_i[:n_tok] <= col_i[:n_tok], first=True)
            update(1, hd, kb.at[:2 * n_tok], vb.at[:2 * n_tok], row_i <= col_i + n_tok, first=True)
        for ch in range(3):
            @pl.when(layer > 0)
            def _():
                take_pass(ch)
                take_n1(ch)
            if ch == 2:
                take_n1(3)
                take_f2(0)
            convert(layer + 1, (ch,))

        @pl.when(layer + 2 < n_layers)
        def _():
            for i in range(3):
                raw_copy(layer + 2, i).start()

        take_n1(4)
        take_f2(1)
        for ch in range(N_1):
            d_n1[ch].wait_recv()
        kv_rows(0, 2 * N_T1)
        take_f2(2)
        for ch in range(n_2):
            d_f2[ch].wait_recv()
        kv_rows(2 * N_T1, 2 * n_t2)
        take_late(0)
        attend(0, 2 * n_tok)
        for g in range(n_2):
            side_late(g)
            if g == n_2 - 2:
                take_late(g + 1)
            kv_rows(*groups[g][:2])
            if g < n_2 - 2:
                take_late(g + 1)
            if g < n_2 - 1:
                attend(*groups[g][:2])

        def put(qi, dst):
            for hd in range(n_heads // 2):
                dst[:, pl.ds(hd * head_dim, head_dim)] = output_rows(hd, pl.ds(pl.multiple_of(qi * n_tok, n_tok), n_tok))

        attend(*groups[n_2 - 1][:2], which=(other,))
        put(other, osend)
        oc.start()
        attend(*groups[n_2 - 1][:2], which=(core,))
        put(core, obuf.at[core])
        out_own(layer)
        for group in (t1_own, t1_fwd, t2_own, t2_relay, t2_fwd, d_n1, d_f1, d_n2, d_f2, [d_own]):
            for cp in group:
                cp.wait_send()
        oc.wait_recv()
        go_on = layer + 1 < n_layers - 1
        later1, later2, later_own = own_copies(layer + 1)
        out_other(layer, 0, N_T1)

        @pl.when(go_on)
        def _():
            launch1()
            for cp in later1:
                cp.start()
        out_other(layer, N_T1, n_t2)

        @pl.when(go_on)
        def _():
            launch2()
            for cp in later2:
                cp.start()
            later_own.start()
        oc.wait_send()
        return carry

    lax.fori_loop(0, n_layers - 1, local_layer, 0)

    last = n_layers - 1
    slot = last % 2
    per_core = n_heads // 2
    main = core == px // per_core
    launch1()
    launch2()
    d_own = ici(last, 0, hown.at[mine], hown.at[mine], chip, other)
    d_own.start()
    m_st[...] = jnp.full(m_st.shape, NEG_BIG, F32)
    l_st[...] = jnp.zeros(l_st.shape, F32)
    acc[...] = jnp.zeros(acc.shape, F32)

    def rcopy(src, dst, send_sem, recv_sem, target):
        return pltpu.make_async_remote_copy(src, dst, send_sem, recv_sem, device_id=target, device_id_type=pl.DeviceIdType.MESH)

    def rel_to(hd):
        return (px - hd + side) % side

    def heads():
        return [(j, core * per_core + j) for j in range(per_core)]

    def half_rows(b):
        return pl.ds(pl.multiple_of(b * n_tok, n_tok), n_tok)

    def kv_send(j, hd, b):
        rel = rel_to(hd)
        return rcopy(st.at[j, :, half_rows(b)], kvg.at[chip, :, half_rows(b)], kv_s.at[j * 2 + b], kv_r.at[rel * 2 + b], dev(at_xy(hd, py)))

    def own_y(way, b):
        ref = kvg.at[chip, :, half_rows(b)]
        return rcopy(ref, ref, kv_s.at[2 * per_core + way * 2 + b], kv_r.at[2 * n_heads + way * 2 + b], dev(yp if way == 0 else ym))

    def half_in(c, i, b):
        ref = kvg.at[c, :, half_rows(b)]
        return rcopy(ref, ref, kv_s.at[0], kv_r.at[i * 2 + b], dev(chip, other))

    def q_send(j, hd, k):
        i = per_core + 2 * j + k
        return rcopy(qst.at[j, k], qg.at[px], st_s.at[i], q_r.at[rel_to(hd)], dev(at_xy(hd, py), k))

    def q_side(j):
        i = per_core + 2 * per_core + j
        return rcopy(qst.at[j, other], qg.at[px], st_s.at[i], q_r.at[0], dev(chip, other))

    def block_chip(dx, dy):
        return at_xy(px + dx, py + dy)

    def y_copy(dx, kind):
        if kind < 2:
            ref = kvg.at[block_chip(dx, 0)]
        else:
            ref = kvg.at[block_chip(dx, -1 if kind == 2 else 1), kind - 2]
        i = dx * 4 + kind
        return rcopy(ref, ref, ys.at[i], yr.at[i], dev(yp if kind % 2 == 0 else ym))

    def to_side(dx, dy):
        ref = kvg.at[block_chip(dx, dy)]
        i = dx * side + dy
        return rcopy(ref, ref, ds.at[i], dr.at[i], dev(chip, other))

    def own_kv(b):
        seg = pl.ds(pl.multiple_of(b * n_tok, n_tok), n_tok)
        rows = hown[seg, :]
        for j in range(per_core):
            cols = pl.ds(j * head_dim, head_dim)
            for i in range(2):
                st[j, i, seg, :] = jnp.dot(rows, wc[slot, 1 + i, :, cols], preferred_element_type=F32).astype(BF16)

    def own_q(b):
        rows = hown[pl.ds(pl.multiple_of(b * n_tok, n_tok), n_tok), :]
        for j in range(per_core):
            cols = pl.ds(j * head_dim, head_dim)
            val = jnp.dot(rows, wc[slot, 0, :, cols], preferred_element_type=F32).astype(BF16)
            qst[j, b] = (val * BF16(scale)).T

    def send_half(b):
        for j, hd in heads():
            @pl.when(hd == px)
            def _():
                kvg[chip, :, half_rows(b)] = st[j, :, half_rows(b)]
                for way in range(2):
                    own_y(way, b).start()

            @pl.when((hd != px) & (rel_to(hd) != 2))
            def _():
                kv_send(j, hd, b).start()

    own_kv(core)
    send_half(core)
    d_own.wait_recv()
    own_kv(other)
    send_half(other)

    @pl.when(main)
    def _():
        to_side(0, 0).start()
    own_q(core)
    own_q(other)
    for j, hd in heads():
        @pl.when(rel_to(hd) == 2)
        def _():
            for b in range(2):
                kv_send(j, hd, b).start()
    for j, hd in heads():
        @pl.when(hd == px)
        def _():
            q_side(j).start()
            qg[px] = qst[j, core]

        @pl.when(hd != px)
        def _():
            for k in range(2):
                q_send(j, hd, k).start()

    def arrive(what, dx):
        @pl.when(main)
        def _():
            if what == "row":
                for b in range(2):
                    half_in(block_chip(dx, 0), dx, b).wait_recv()
                y_copy(dx, 0).start()
                y_copy(dx, 1).start()
                to_side(dx, 0).start()
            elif what == "y":
                for kind in range(2):
                    if dx:
                        y_copy(dx, kind).wait_recv()
                    else:
                        for b in range(2):
                            half_in(block_chip(0, -1 if kind == 0 else 1), n_heads + kind, b).wait_recv()
                for kind in range(2, 4):
                    y_copy(dx, kind).start()
                to_side(dx, side - 1).start()
                to_side(dx, 1).start()
            else:
                for kind in range(2, 4):
                    rcopy(kvg.at[block_chip(dx, 2), kind - 2], kvg.at[block_chip(dx, 2), kind - 2], ys.at[dx * 4 + kind],
                          yr.at[dx * 4 + kind], dev(chip, other)).wait_recv()
                to_side(dx, 2).start()

    def have(dx, dy, i):
        @pl.when(jnp.logical_not(main))
        def _():
            c = block_chip(dx, dy)
            rcopy(kvg.at[c], kvg.at[c], ds.at[i], dr.at[i], dev(chip, other)).wait_recv()

    arrive("row", 1)
    arrive("row", side - 1)
    arrive("y", 0)
    arrive("row", 2)
    for dx in range(side):
        q_in = rcopy(qst.at[0, 0], qg.at[(px + dx) % side], st_s.at[0], q_r.at[dx], dev(chip, other))
        if dx == 0:
            @pl.when(jnp.logical_not(main))
            def _():
                q_in.wait_recv()
        else:
            q_in.wait_recv()

    def q_cols_of(b):
        return pl.ds(pl.multiple_of(b % 2 * n_tok, n_tok), n_tok)

    key_i = lax.broadcasted_iota(jnp.int32, (2 * n_tok, n_tok), 0)
    query_i = lax.broadcasted_iota(jnp.int32, (2 * n_tok, n_tok), 1) + core * n_tok

    def row_step(dx, carry):
        src_x = (px + dx) % side
        have(dx, 0, dx * side)
        c = block_chip(dx, 0)

        def one(b, c2):
            @pl.when(src_x <= b)
            def _():
                mask = key_i - query_i <= (b - src_x) * (2 * n_tok)
                soft_step(kvg[c, 0], qg[b], kvg[c, 1], b // 2, q_cols_of(b), mask)
            return c2

        lax.fori_loop(0, side, one, 0)
        return carry

    lax.fori_loop(0, side, row_step, 0)

    def block_step(i, carry):
        for (what, col), when in ARRIVE_AT.items():
            @pl.when(i == when)
            def _():
                arrive(what, col)
        dx = table(i, [blk[0] for blk in BLOCKS])
        dy = table(i, [blk[1] for blk in BLOCKS])
        have(dx, dy, dx * side + dy)
        c = block_chip(dx, dy)

        @pl.when(c // side < py)
        def _():
            for b in range(side):
                soft_step(kvg[c, 0], qg[b], kvg[c, 1], b // 2, pl.ds(b % 2 * n_tok, n_tok))
        return carry

    lax.fori_loop(0, len(BLOCKS), block_step, 0)

    def o_send(rel):
        b = (px + rel) % side
        return rcopy(qst.at[rel // 2, rel % 2], og.at[px], o_s.at[rel], o_r.at[rel], dev(at_xy(px + rel, py)))

    def o_in(rel):
        ref = og.at[(px - rel + side) % side]
        return rcopy(ref, ref, o_s.at[rel], o_r.at[rel], dev(chip, other))

    for j, hd in heads():
        @pl.when(hd == px)
        def _():
            q_side(j).wait_send()

        @pl.when(hd != px)
        def _():
            for k in range(2):
                kv_send(j, hd, k).wait_send()
                q_send(j, hd, k).wait_send()
    for rel in (2, 1, 3, 0):
        b = (px + rel) % side
        val = output_rows(b // 2, q_cols_of(b))
        if rel:
            qst[rel // 2, rel % 2] = val
            o_send(rel).start()
        else:
            og[px] = val
    wo_copy(last).wait()
    wide = d_model // 3
    for rel in (0, 1, 3, 2):
        if rel:
            o_in(rel).wait_recv()
        head = (px - rel + side) % side
        rows = pl.ds(pl.multiple_of(head * head_dim, head_dim), head_dim)
        for j in range(3):
            cols = pl.ds(j * wide, wide)
            prod = jnp.dot(og[head], wob[slot, rows, cols], preferred_element_type=F32)
            if rel == 0:
                part[:, cols] = prod
            elif rel != 2:
                part[:, cols] = part[:, cols] + prod
            else:
                out[:, cols] = (xb[:, cols].astype(F32) + (part[:, cols] + prod)).astype(BF16)
    d_own.wait_send()
    for rel in range(1, side):
        o_send(rel).wait_send()

    @pl.when(main)
    def _():
        for way in range(2):
            for b in range(2):
                own_y(way, b).wait_send()
        for dx in range(side):
            for kind in range(0 if dx else 2, 4):
                y_copy(dx, kind).wait_send()
            for dy in range(side):
                to_side(dx, dy).wait_send()


def solution(mesh):
    n_cp = mesh.shape["cp"]

    def device_body(hidden, w_query, w_key, w_value, w_out):
        n_tok, d_model = hidden.shape
        n_layers, n_heads, head_dim, _ = w_out.shape
        half_w = n_heads // 2 * head_dim
        n_loc = n_layers - 1
        n_t2 = n_tok - N_T1
        flat = n_heads * head_dim // LANES * d_model
        n_copy = (4 * N_T1 + 5 * n_t2) // PIECE + 2
        vmem = pl.BlockSpec(memory_space=pltpu.VMEM)
        hbm = pl.BlockSpec(memory_space=pl.ANY)
        scratch = [
            pltpu.VMEM((n_tok, d_model), BF16),
            pltpu.VMEM((2 * n_tok, d_model), BF16),
            pltpu.VMEM((n_loc, 4 * n_tok, d_model), BF16),
            pltpu.VMEM((4 * n_tok, LANES), jnp.int32),
            pltpu.VMEM((n_loc, n_t2, d_model), BF16),
            pltpu.VMEM((n_cp // 2, 2, 2 * n_tok, head_dim), BF16),
            pltpu.VMEM((n_heads // 2, 2, 2 * n_tok, head_dim), BF16),
            pltpu.VMEM((n_heads // 2, 2, head_dim, n_tok), BF16),
            pltpu.VMEM((n_heads, head_dim, n_tok), BF16),
            pltpu.VMEM((n_heads, n_tok, head_dim), BF16),
            pltpu.VMEM((3, flat, LANES), BF16),
            pltpu.VMEM((n_heads * head_dim, LANES), F32),
            pltpu.VMEM((2, 3, d_model, half_w), BF16),
            pltpu.VMEM((2, n_heads * head_dim, d_model), BF16),
            pltpu.VMEM((half_w, 2 * n_tok), BF16),
            pltpu.VMEM((6 * n_tok, half_w), BF16),
            pltpu.VMEM((6 * n_tok, half_w), BF16),
            pltpu.VMEM((n_heads // 2, head_dim, 2 * n_tok), F32),
            pltpu.VMEM((n_heads // 2, 8, 2 * n_tok), F32),
            pltpu.VMEM((n_heads // 2, 8, 2 * n_tok), F32),
            pltpu.VMEM((2, n_tok, half_w), BF16),
            pltpu.VMEM((n_tok, half_w), BF16),
            pltpu.VMEM((n_tok, d_model), F32),
            pltpu.SemaphoreType.DMA((4,)),
            pltpu.SemaphoreType.DMA((2,)),
            pltpu.SemaphoreType.DMA((n_layers, n_copy)),
            pltpu.SemaphoreType.DMA((n_layers, n_copy)),
            pltpu.SemaphoreType.DMA((n_heads // 2 * 4,)),
            pltpu.SemaphoreType.DMA((n_heads + 4,)),
            pltpu.SemaphoreType.DMA((2 * n_heads + 4,)),
            pltpu.SemaphoreType.DMA((n_heads,)),
            pltpu.SemaphoreType.DMA((n_cp // 2,)),
            pltpu.SemaphoreType.DMA((n_cp // 2,)),
            pltpu.SemaphoreType.DMA((n_cp // 2,)),
            pltpu.SemaphoreType.DMA((n_cp // 2,)),
            pltpu.SemaphoreType.DMA((n_heads,)),
            pltpu.SemaphoreType.DMA((n_heads,)),
        ]
        return pl.pallas_call(
            functools.partial(kernel, n_cp, n_layers, n_heads, head_dim),
            out_shape=jax.ShapeDtypeStruct(hidden.shape, hidden.dtype),
            in_specs=[hbm, hbm, hbm, hbm, hbm],
            out_specs=vmem,
            scratch_shapes=scratch,
            compiler_params=pltpu.CompilerParams(collective_id=0, has_side_effects=True, vmem_limit_bytes=66_500_000),
        )(hidden, flat_view(w_query), flat_view(w_key), flat_view(w_value),
          w_out.reshape(n_layers, n_heads * head_dim, d_model))

    row_spec = P(("dp", "cp"), None)
    return jax.shard_map(device_body, mesh=mesh, in_specs=(row_spec, P(), P(), P(), P()), out_specs=row_spec, check_vma=False)
```

```python
import functools
import math

import jax
import jax.numpy as jnp
from jax import lax
from jax.experimental import pallas as pl
from jax.experimental.pallas import tpu as pltpu
from jax.sharding import PartitionSpec as P

WINDOW = 1024
NORM_EPS = 1e-6
NEG_BIG = -1e30
BF16 = jnp.bfloat16
F32 = jnp.float32
LANES = 128
N_T1 = 160
PIECE = 32
N_1 = N_T1 // PIECE

BLOCKS = ((0, 1), (0, 3), (1, 1), (1, 3), (0, 2), (3, 1), (3, 3), (2, 1), (2, 3), (1, 2), (3, 2), (2, 2))
ARRIVE_AT = {("y", 1): 0, ("opp", 0): 3, ("y", 3): 4, ("y", 2): 6, ("opp", 1): 8, ("opp", 3): 9, ("opp", 2): 10}


def flat_view(weight):
    n_layers, d_model, n_heads, head_dim = weight.shape
    split = weight.reshape(n_layers, d_model, n_heads, head_dim // LANES, LANES)
    return split.transpose(0, 1, 3, 2, 4).reshape(n_layers, -1, LANES)


def table(index, values):
    out = jnp.int32(values[0])
    for pos, value in enumerate(values):
        if pos and value != values[0]:
            out = jnp.where(index == pos, jnp.int32(value), out)
    return out


def kernel(n_cp, n_layers, n_heads, head_dim, x_in, wq, wk, wv, wo, out,
           xb, hown, hh, tk, relay, kvg, st, qst, qg, og, raw, fs, wc, wob, qt, kb, vb,
           acc, m_st, l_st, obuf, osend, part,
           raw_sem, wo_sem, ls, lr, st_s, kv_s, kv_r, q_r, ys, yr, ds, dr, o_s, o_r):
    n_tok, d_model = x_in.shape
    n_chip = n_cp // 2
    side = math.isqrt(n_chip)
    half_w = n_heads // 2 * head_dim
    n_ct = head_dim // LANES
    n_t2 = n_tok - N_T1
    scale = head_dim ** -0.5
    me = lax.axis_index("cp")
    chip = me // 2
    core = me % 2
    other = 1 - core
    px, py = chip % side, chip // side

    def at_xy(x, y):
        return ((y + side) % side) * side + (x + side) % side

    def ring(step):
        return (chip + n_chip + step) % n_chip

    def dev(c, k=None):
        return {"cp": c * 2 + (core if k is None else k)}

    nxt, prv = ring(1), ring(-1)
    xm, xp = at_xy(px - 1, py), at_xy(px + 1, py)
    ym, yp = at_xy(px, py - 1), at_xy(px, py + 1)

    def pass_to(c):
        x, y = c % side, c // side
        return at_xy(x - 1, y + jnp.where(x == 2, 1, 0))

    via = pass_to(chip)
    via_from = at_xy(px + 1, py - jnp.where(px == 1, 1, 0))
    skip_to = (via_from + 2) % n_chip
    skip_from = pass_to(ring(-2))

    barrier = pltpu.get_barrier_semaphore()
    peers = [dev(c) for c in (nxt, prv, ym, yp, via, via_from, skip_to, skip_from)] + [dev(chip, other)]
    peers += [dev(at_xy(px + d, py), k) for d in range(1, side) for k in range(2)]
    for peer in peers:
        pl.semaphore_signal(barrier, inc=1, device_id=peer, device_id_type=pl.DeviceIdType.MESH)

    def raw_copy(layer, i):
        return pltpu.make_async_copy((wq, wk, wv)[i].at[layer], raw.at[i], raw_sem.at[i])

    def wo_copy(layer):
        slot = layer % 2
        return pltpu.make_async_copy(wo.at[layer], wob.at[slot], wo_sem.at[slot])

    x_copy = pltpu.make_async_copy(x_in, xb, raw_sem.at[3])
    x_copy.start()
    for i in range(3):
        raw_copy(0, i).start()
    wo_copy(0).start()

    def convert(layer, which=(0, 1, 2)):
        slot = layer % 2
        d_step = fs.shape[0] // (n_heads * n_ct)
        for i in which:
            raw_copy(layer, i).wait()

            def chunk(j, carry):
                r0 = pl.multiple_of(j * fs.shape[0], fs.shape[0])
                d0 = pl.multiple_of(j * d_step, d_step)
                fs[...] = raw[i, pl.ds(r0, fs.shape[0]), :].astype(F32)
                for hd in range(n_heads // 2):
                    for ct in range(n_ct):
                        first = ct * n_heads + core * (n_heads // 2) + hd
                        piece = fs[pl.ds(first, d_step, stride=n_heads * n_ct), :]
                        wc[slot, i, pl.ds(d0, d_step), pl.ds(hd * head_dim + ct * LANES, LANES)] = piece.astype(BF16)
                return carry
            lax.fori_loop(0, d_model // d_step, chunk, 0)

    def project(rows, slot, which, dst):
        for j in range(half_w // head_dim):
            cols = pl.ds(j * head_dim, head_dim)
            dst[:, cols] = jnp.dot(rows, wc[slot, which, :, cols], preferred_element_type=F32).astype(BF16)

    def project_q(rows, slot, q_cols):
        for j in range(half_w // head_dim):
            cols = pl.ds(j * head_dim, head_dim)
            val = jnp.dot(rows, wc[slot, 0, :, cols], preferred_element_type=F32).astype(BF16)
            qt[cols, q_cols] = (val * BF16(scale)).T

    def soft_step(k_val, q_val, v_val, hd, q_cols, mask=None, first=False):
        s = jnp.dot(k_val, q_val, preferred_element_type=F32)
        if mask is not None:
            s = jnp.where(mask, s, NEG_BIG)
        new_m = jnp.max(s, axis=0, keepdims=True)
        if not first:
            old_m = m_st[hd, :1, q_cols]
            new_m = jnp.maximum(old_m, new_m)
        p = jnp.exp(s - new_m)
        part_sum = jnp.sum(p.reshape(p.shape[0] // 8, 8, p.shape[1]), axis=0)
        pv = lax.dot_general(v_val, p.astype(BF16), (((0,), (0,)), ((), ())), preferred_element_type=F32)
        if first:
            l_st[hd, :, q_cols] = part_sum
            acc[hd, :, q_cols] = pv
        else:
            alpha = jnp.exp(old_m - new_m)
            l_st[hd, :, q_cols] = l_st[hd, :, q_cols] * alpha + part_sum
            acc[hd, :, q_cols] = acc[hd, :, q_cols] * alpha + pv
        m_st[hd, :1, q_cols] = new_m

    def update(qi, hd, k_ref, v_ref, mask=None, first=False):
        dims = pl.ds(hd * head_dim, head_dim)
        q_cols = pl.ds(qi * n_tok if isinstance(qi, int) else pl.multiple_of(qi * n_tok, n_tok), n_tok)
        soft_step(k_ref[:, dims], qt[dims, q_cols], v_ref[:, dims], hd, q_cols, mask, first)

    def update_all(k_ref, v_ref, mask_of=None, which=(0, 1)):
        for qi in which:
            mask = None if mask_of is None else mask_of(qi)
            for hd in range(n_heads // 2):
                update(qi, hd, k_ref, v_ref, mask)

    def output_rows(hd, q_cols):
        total = jnp.sum(l_st[hd, :, q_cols], axis=0, keepdims=True)
        return (acc[hd, :, q_cols] / total).astype(BF16).T

    def normed(lo=0, n=n_tok):
        xf = xb[lo:lo + n, :].astype(F32)
        return (xf * lax.rsqrt(jnp.mean(xf * xf, axis=-1, keepdims=True) + NORM_EPS)).astype(BF16)

    def o_copy(layer):
        return pltpu.make_async_remote_copy(osend, obuf.at[core], ls.at[layer, ls.shape[1] - 1], lr.at[layer, lr.shape[1] - 1],
                                            device_id=dev(chip, other), device_id_type=pl.DeviceIdType.MESH)

    def out_own(layer):
        slot = layer % 2
        wo_copy(layer).wait()
        wide = d_model // 3
        mine = pl.ds(pl.multiple_of(core * half_w, half_w), half_w)
        for j in range(3):
            cols = pl.ds(j * wide, wide)
            part[:, cols] = jnp.dot(obuf[core], wob[slot, mine, cols], preferred_element_type=F32)

    def out_other(layer, lo, n):
        slot = layer % 2
        wide = d_model // 3
        theirs = pl.ds(pl.multiple_of(other * half_w, half_w), half_w)
        for j in range(3):
            cols = pl.ds(j * wide, wide)
            prod = part[lo:lo + n, cols] + jnp.dot(obuf[other, lo:lo + n, :], wob[slot, theirs, cols], preferred_element_type=F32)
            xb[lo:lo + n, cols] = (xb[lo:lo + n, cols].astype(F32) + prod).astype(BF16)

    def ici(layer, i, src, dst, c, k=None):
        return pltpu.make_async_remote_copy(src, dst, ls.at[layer, i], lr.at[layer, i],
                                            device_id=dev(c, k), device_id_type=pl.DeviceIdType.MESH)

    n_2 = n_t2 // PIECE
    both = 2 * PIECE
    off_near1 = [ch * both for ch in range(N_1)]
    off_far2 = [2 * N_T1 + ch * both for ch in range(n_2)]
    off_near2, off_far1, groups = [], [], []
    at_row = 2 * n_tok
    per = -(-N_1 // n_2)
    for ch in range(n_2):
        first = at_row
        off_near2.append(at_row)
        at_row += both
        far_ids = list(range(ch * per, min(N_1, (ch + 1) * per)))
        for _ in far_ids:
            off_far1.append(at_row)
            at_row += both
        groups.append((first, at_row - first, far_ids))
    key_i = lax.broadcasted_iota(jnp.int32, tk.shape, 0)
    limit = jnp.full(tk.shape, 4 * n_tok, jnp.int32)
    for offs, base in ((off_far1, 0), (off_far2, N_T1)):
        for ch, off in enumerate(offs):
            for k in range(2):
                start = off + k * PIECE
                inside = (key_i >= start) & (key_i < start + PIECE)
                shift = k * n_tok + base + ch * PIECE + WINDOW - 4 * n_tok - start
                limit = jnp.where(inside, jnp.where(chip >= 2, key_i + shift, -1), limit)
    tk[...] = limit

    mine = pl.ds(pl.multiple_of(core * n_tok, n_tok), n_tok)

    def own_rows(lo, n):
        return hown.at[pl.ds(pl.multiple_of(core * n_tok + lo, 16), n), :]

    def own_copies(layer):
        hl = hh.at[layer]
        t1 = [ici(layer, ch, own_rows(ch * PIECE, PIECE), hl.at[piece_rows(off), :], nxt) for ch, off in enumerate(off_near1)]
        t2 = [ici(layer, N_1 + ch, own_rows(N_T1 + ch * PIECE, PIECE), relay.at[layer, pl.ds(ch * PIECE, PIECE), :], via)
              for ch in range(n_2)]
        side_own = ici(layer, N_1 + n_2, hown.at[mine], hown.at[mine], chip, other)
        return t1, t2, side_own

    def piece_rows(off):
        return pl.ds(pl.multiple_of(off + core * PIECE, 16), PIECE)

    def launch1():
        hown[pl.ds(pl.multiple_of(core * n_tok, n_tok), N_T1), :] = normed(0, N_T1)

    def launch2():
        hown[pl.ds(pl.multiple_of(core * n_tok + N_T1, 16), n_t2), :] = normed(N_T1, n_t2)

    def local_layer(layer, carry):
        slot = layer % 2
        t1_own, t2_own, d_own = own_copies(layer)
        base = N_1 + n_2 + 1

        def piece(off):
            return hh.at[layer, piece_rows(off), :]

        near1, far1 = [piece(off) for off in off_near1], [piece(off) for off in off_far1]
        near2, far2 = [piece(off) for off in off_near2], [piece(off) for off in off_far2]
        pass2 = [relay.at[layer, pl.ds(ch * PIECE, PIECE), :] for ch in range(n_2)]

        def series(srcs, dsts, c, k=None):
            nonlocal base
            out = [ici(layer, base + i, a, b, c, k) for i, (a, b) in enumerate(zip(srcs, dsts))]
            base += len(out)
            return out

        t1_fwd = series(near1, far1, nxt)
        t2_relay = series(pass2, far2, skip_to)
        t2_fwd = series(far2, near2, prv)
        d_n1 = series(near1, near1, chip, other)
        d_f1 = series(far1, far1, chip, other)
        d_n2 = series(near2, near2, chip, other)
        d_f2 = series(far2, far2, chip, other)
        oc = o_copy(layer)

        @pl.when(layer == 0)
        def _():
            x_copy.wait()
            launch1()
            pl.semaphore_wait(barrier, len(peers))
            for cp in t1_own:
                cp.start()
            launch2()
            for cp in t2_own:
                cp.start()
            d_own.start()
        wo_copy(layer + 1).start()

        def own_block(b):
            dst_rows = pl.ds(pl.multiple_of(b * n_tok, n_tok), n_tok)
            rows = hown[dst_rows, :]
            project_q(rows, slot, dst_rows)
            project(rows, slot, 1, kb.at[dst_rows])
            project(rows, slot, 2, vb.at[dst_rows])

        def take(arrived, onward, side_copy):
            arrived.wait_recv()
            if onward is not None:
                onward.start()
            if side_copy is not None:
                side_copy.start()

        def take_n1(ch):
            take(t1_own[ch], t1_fwd[ch], d_n1[ch])

        def take_pass(ch):
            take(t2_own[ch], t2_relay[ch], None)

        def take_f2(ch):
            take(t2_relay[ch], t2_fwd[ch], d_f2[ch])

        def take_late(g):
            for ch in groups[g][2]:
                take(t1_fwd[ch], None, d_f1[ch])
            take(t2_fwd[g], None, d_n2[g])

        def side_late(g):
            for ch in groups[g][2]:
                d_f1[ch].wait_recv()
            d_n2[g].wait_recv()

        def kv_rows(lo, n):
            @pl.when(chip >= 1)
            def _():
                rows = hh[layer, lo:lo + n]
                project(rows, slot, 1, kb.at[pl.ds(2 * n_tok + lo, n)])
                project(rows, slot, 2, vb.at[pl.ds(2 * n_tok + lo, n)])

        lane_i = lax.broadcasted_iota(jnp.int32, (1, n_tok), 1)

        def attend(lo, n, which=(0, 1)):
            def mask_of(qi):
                rows = tk[lo:lo + n, :]
                return jnp.concatenate([rows] * (n_tok // LANES), axis=1) > lane_i + qi * n_tok

            @pl.when(chip >= 1)
            def _():
                at = pl.ds(2 * n_tok + lo, n)
                update_all(kb.at[at], vb.at[at], mask_of, which)

        @pl.when(layer == 0)
        def _():
            for ch in range(3):
                convert(0, (ch,))
                take_pass(ch)
                take_n1(ch)
            for i in range(3):
                raw_copy(1, i).start()

        own_block(core)
        d_own.wait_recv()
        own_block(other)
        row_i = lax.broadcasted_iota(jnp.int32, (2 * n_tok, n_tok), 0)
        col_i = lax.broadcasted_iota(jnp.int32, (2 * n_tok, n_tok), 1)
        for hd in range(n_heads // 2):
            update(0, hd, kb.at[:n_tok], vb.at[:n_tok], row_i[:n_tok] <= col_i[:n_tok], first=True)
            update(1, hd, kb.at[:2 * n_tok], vb.at[:2 * n_tok], row_i <= col_i + n_tok, first=True)
        for ch in range(3):
            @pl.when(layer > 0)
            def _():
                take_pass(ch)
                take_n1(ch)
            if ch == 2:
                take_n1(3)
                take_f2(0)
            convert(layer + 1, (ch,))

        @pl.when(layer + 2 < n_layers)
        def _():
            for i in range(3):
                raw_copy(layer + 2, i).start()

        take_n1(4)
        take_f2(1)
        for ch in range(N_1):
            d_n1[ch].wait_recv()
        kv_rows(0, 2 * N_T1)
        take_f2(2)
        for ch in range(n_2):
            d_f2[ch].wait_recv()
        kv_rows(2 * N_T1, 2 * n_t2)
        take_late(0)
        attend(0, 2 * n_tok)
        for g in range(n_2):
            side_late(g)
            if g == n_2 - 2:
                take_late(g + 1)
            kv_rows(*groups[g][:2])
            if g < n_2 - 2:
                take_late(g + 1)
            if g < n_2 - 1:
                attend(*groups[g][:2])

        def put(qi, dst):
            for hd in range(n_heads // 2):
                dst[:, pl.ds(hd * head_dim, head_dim)] = output_rows(hd, pl.ds(pl.multiple_of(qi * n_tok, n_tok), n_tok))

        attend(*groups[n_2 - 1][:2], which=(other,))
        put(other, osend)
        oc.start()
        attend(*groups[n_2 - 1][:2], which=(core,))
        put(core, obuf.at[core])
        out_own(layer)
        for group in (t1_own, t1_fwd, t2_own, t2_relay, t2_fwd, d_n1, d_f1, d_n2, d_f2, [d_own]):
            for cp in group:
                cp.wait_send()
        oc.wait_recv()
        go_on = layer + 1 < n_layers - 1
        later1, later2, later_own = own_copies(layer + 1)
        out_other(layer, 0, N_T1)

        @pl.when(go_on)
        def _():
            launch1()
            for cp in later1:
                cp.start()
        out_other(layer, N_T1, n_t2)

        @pl.when(go_on)
        def _():
            launch2()
            for cp in later2:
                cp.start()
            later_own.start()
        oc.wait_send()
        return carry

    lax.fori_loop(0, n_layers - 1, local_layer, 0)

    last = n_layers - 1
    slot = last % 2
    per_core = n_heads // 2
    main = core == px // per_core
    launch1()
    launch2()
    d_own = ici(last, 0, hown.at[mine], hown.at[mine], chip, other)
    d_own.start()
    m_st[...] = jnp.full(m_st.shape, NEG_BIG, F32)
    l_st[...] = jnp.zeros(l_st.shape, F32)
    acc[...] = jnp.zeros(acc.shape, F32)

    def rcopy(src, dst, send_sem, recv_sem, target):
        return pltpu.make_async_remote_copy(src, dst, send_sem, recv_sem, device_id=target, device_id_type=pl.DeviceIdType.MESH)

    def rel_to(hd):
        return (px - hd + side) % side

    def heads():
        return [(j, core * per_core + j) for j in range(per_core)]

    def half_rows(b):
        return pl.ds(pl.multiple_of(b * n_tok, n_tok), n_tok)

    def kv_send(j, hd, b):
        rel = rel_to(hd)
        return rcopy(st.at[j, :, half_rows(b)], kvg.at[chip, :, half_rows(b)], kv_s.at[j * 2 + b], kv_r.at[rel * 2 + b], dev(at_xy(hd, py)))

    def own_y(way, b):
        ref = kvg.at[chip, :, half_rows(b)]
        return rcopy(ref, ref, kv_s.at[2 * per_core + way * 2 + b], kv_r.at[2 * n_heads + way * 2 + b], dev(yp if way == 0 else ym))

    def half_in(c, i, b):
        ref = kvg.at[c, :, half_rows(b)]
        return rcopy(ref, ref, kv_s.at[0], kv_r.at[i * 2 + b], dev(chip, other))

    def q_send(j, hd, k):
        i = per_core + 2 * j + k
        return rcopy(qst.at[j, k], qg.at[px], st_s.at[i], q_r.at[rel_to(hd)], dev(at_xy(hd, py), k))

    def q_side(j):
        i = per_core + 2 * per_core + j
        return rcopy(qst.at[j, other], qg.at[px], st_s.at[i], q_r.at[0], dev(chip, other))

    def block_chip(dx, dy):
        return at_xy(px + dx, py + dy)

    def y_copy(dx, kind):
        if kind < 2:
            ref = kvg.at[block_chip(dx, 0)]
        else:
            ref = kvg.at[block_chip(dx, -1 if kind == 2 else 1), kind - 2]
        i = dx * 4 + kind
        return rcopy(ref, ref, ys.at[i], yr.at[i], dev(yp if kind % 2 == 0 else ym))

    def to_side(dx, dy):
        ref = kvg.at[block_chip(dx, dy)]
        i = dx * side + dy
        return rcopy(ref, ref, ds.at[i], dr.at[i], dev(chip, other))

    def own_kv(b):
        seg = pl.ds(pl.multiple_of(b * n_tok, n_tok), n_tok)
        rows = hown[seg, :]
        for j in range(per_core):
            cols = pl.ds(j * head_dim, head_dim)
            for i in range(2):
                st[j, i, seg, :] = jnp.dot(rows, wc[slot, 1 + i, :, cols], preferred_element_type=F32).astype(BF16)

    def own_q(b):
        rows = hown[pl.ds(pl.multiple_of(b * n_tok, n_tok), n_tok), :]
        for j in range(per_core):
            cols = pl.ds(j * head_dim, head_dim)
            val = jnp.dot(rows, wc[slot, 0, :, cols], preferred_element_type=F32).astype(BF16)
            qst[j, b] = (val * BF16(scale)).T

    def send_half(b):
        for j, hd in heads():
            @pl.when(hd == px)
            def _():
                kvg[chip, :, half_rows(b)] = st[j, :, half_rows(b)]
                for way in range(2):
                    own_y(way, b).start()

            @pl.when((hd != px) & (rel_to(hd) != 2))
            def _():
                kv_send(j, hd, b).start()

    own_kv(core)
    send_half(core)
    d_own.wait_recv()
    own_kv(other)
    send_half(other)

    @pl.when(main)
    def _():
        to_side(0, 0).start()
    own_q(core)
    own_q(other)
    for j, hd in heads():
        @pl.when(rel_to(hd) == 2)
        def _():
            for b in range(2):
                kv_send(j, hd, b).start()
    for j, hd in heads():
        @pl.when(hd == px)
        def _():
            q_side(j).start()
            qg[px] = qst[j, core]

        @pl.when(hd != px)
        def _():
            for k in range(2):
                q_send(j, hd, k).start()

    def arrive(what, dx):
        @pl.when(main)
        def _():
            if what == "row":
                for b in range(2):
                    half_in(block_chip(dx, 0), dx, b).wait_recv()
                y_copy(dx, 0).start()
                y_copy(dx, 1).start()
                to_side(dx, 0).start()
            elif what == "y":
                for kind in range(2):
                    if dx:
                        y_copy(dx, kind).wait_recv()
                    else:
                        for b in range(2):
                            half_in(block_chip(0, -1 if kind == 0 else 1), n_heads + kind, b).wait_recv()
                for kind in range(2, 4):
                    y_copy(dx, kind).start()
                to_side(dx, side - 1).start()
                to_side(dx, 1).start()
            else:
                for kind in range(2, 4):
                    rcopy(kvg.at[block_chip(dx, 2), kind - 2], kvg.at[block_chip(dx, 2), kind - 2], ys.at[dx * 4 + kind],
                          yr.at[dx * 4 + kind], dev(chip, other)).wait_recv()
                to_side(dx, 2).start()

    def have(dx, dy, i):
        @pl.when(jnp.logical_not(main))
        def _():
            c = block_chip(dx, dy)
            rcopy(kvg.at[c], kvg.at[c], ds.at[i], dr.at[i], dev(chip, other)).wait_recv()

    arrive("row", 1)
    arrive("row", side - 1)
    arrive("y", 0)
    arrive("row", 2)
    for dx in range(side):
        q_in = rcopy(qst.at[0, 0], qg.at[(px + dx) % side], st_s.at[0], q_r.at[dx], dev(chip, other))
        if dx == 0:
            @pl.when(jnp.logical_not(main))
            def _():
                q_in.wait_recv()
        else:
            q_in.wait_recv()

    def q_cols_of(b):
        return pl.ds(pl.multiple_of(b % 2 * n_tok, n_tok), n_tok)

    key_i = lax.broadcasted_iota(jnp.int32, (2 * n_tok, n_tok), 0)
    query_i = lax.broadcasted_iota(jnp.int32, (2 * n_tok, n_tok), 1) + core * n_tok

    def row_step(dx, carry):
        src_x = (px + dx) % side
        have(dx, 0, dx * side)
        c = block_chip(dx, 0)

        def one(b, c2):
            @pl.when(src_x <= b)
            def _():
                mask = key_i - query_i <= (b - src_x) * (2 * n_tok)
                soft_step(kvg[c, 0], qg[b], kvg[c, 1], b // 2, q_cols_of(b), mask)
            return c2

        lax.fori_loop(0, side, one, 0)
        return carry

    lax.fori_loop(0, side, row_step, 0)

    def block_step(i, carry):
        for (what, col), when in ARRIVE_AT.items():
            @pl.when(i == when)
            def _():
                arrive(what, col)
        dx = table(i, [blk[0] for blk in BLOCKS])
        dy = table(i, [blk[1] for blk in BLOCKS])
        have(dx, dy, dx * side + dy)
        c = block_chip(dx, dy)

        @pl.when(c // side < py)
        def _():
            for b in range(side):
                soft_step(kvg[c, 0], qg[b], kvg[c, 1], b // 2, pl.ds(b % 2 * n_tok, n_tok))
        return carry

    lax.fori_loop(0, len(BLOCKS) - 1, block_step, 0)
    end_dx, end_dy = BLOCKS[-1]
    have(end_dx, end_dy, end_dx * side + end_dy)
    c_end = block_chip(end_dx, end_dy)

    def o_send(rel):
        b = (px + rel) % side
        return rcopy(qst.at[rel // 2, rel % 2], og.at[px], o_s.at[rel], o_r.at[rel], dev(at_xy(px + rel, py)))

    def o_in(rel):
        ref = og.at[(px - rel + side) % side]
        return rcopy(ref, ref, o_s.at[rel], o_r.at[rel], dev(chip, other))

    for j, hd in heads():
        @pl.when(hd == px)
        def _():
            q_side(j).wait_send()

        @pl.when(hd != px)
        def _():
            for k in range(2):
                kv_send(j, hd, k).wait_send()
                q_send(j, hd, k).wait_send()
    for rel in (2, 1, 3, 0):
        b = (px + rel) % side

        @pl.when(c_end // side < py)
        def _():
            soft_step(kvg[c_end, 0], qg[b], kvg[c_end, 1], b // 2, q_cols_of(b))
        val = output_rows(b // 2, q_cols_of(b))
        if rel:
            qst[rel // 2, rel % 2] = val
            o_send(rel).start()
        else:
            og[px] = val
    wo_copy(last).wait()
    wide = d_model // 3
    for rel in (0, 1, 3, 2):
        if rel:
            o_in(rel).wait_recv()
        head = (px - rel + side) % side
        rows = pl.ds(pl.multiple_of(head * head_dim, head_dim), head_dim)
        for j in range(3):
            cols = pl.ds(j * wide, wide)
            prod = jnp.dot(og[head], wob[slot, rows, cols], preferred_element_type=F32)
            if rel == 0:
                part[:, cols] = prod
            elif rel != 2:
                part[:, cols] = part[:, cols] + prod
            else:
                out[:, cols] = (xb[:, cols].astype(F32) + (part[:, cols] + prod)).astype(BF16)
    d_own.wait_send()
    for rel in range(1, side):
        o_send(rel).wait_send()

    @pl.when(main)
    def _():
        for way in range(2):
            for b in range(2):
                own_y(way, b).wait_send()
        for dx in range(side):
            for kind in range(0 if dx else 2, 4):
                y_copy(dx, kind).wait_send()
            for dy in range(side):
                to_side(dx, dy).wait_send()


def solution(mesh):
    n_cp = mesh.shape["cp"]

    def device_body(hidden, w_query, w_key, w_value, w_out):
        n_tok, d_model = hidden.shape
        n_layers, n_heads, head_dim, _ = w_out.shape
        half_w = n_heads // 2 * head_dim
        n_loc = n_layers - 1
        n_t2 = n_tok - N_T1
        flat = n_heads * head_dim // LANES * d_model
        n_copy = (4 * N_T1 + 5 * n_t2) // PIECE + 2
        vmem = pl.BlockSpec(memory_space=pltpu.VMEM)
        hbm = pl.BlockSpec(memory_space=pl.ANY)
        scratch = [
            pltpu.VMEM((n_tok, d_model), BF16),
            pltpu.VMEM((2 * n_tok, d_model), BF16),
            pltpu.VMEM((n_loc, 4 * n_tok, d_model), BF16),
            pltpu.VMEM((4 * n_tok, LANES), jnp.int32),
            pltpu.VMEM((n_loc, n_t2, d_model), BF16),
            pltpu.VMEM((n_cp // 2, 2, 2 * n_tok, head_dim), BF16),
            pltpu.VMEM((n_heads // 2, 2, 2 * n_tok, head_dim), BF16),
            pltpu.VMEM((n_heads // 2, 2, head_dim, n_tok), BF16),
            pltpu.VMEM((n_heads, head_dim, n_tok), BF16),
            pltpu.VMEM((n_heads, n_tok, head_dim), BF16),
            pltpu.VMEM((3, flat, LANES), BF16),
            pltpu.VMEM((n_heads * head_dim, LANES), F32),
            pltpu.VMEM((2, 3, d_model, half_w), BF16),
            pltpu.VMEM((2, n_heads * head_dim, d_model), BF16),
            pltpu.VMEM((half_w, 2 * n_tok), BF16),
            pltpu.VMEM((6 * n_tok, half_w), BF16),
            pltpu.VMEM((6 * n_tok, half_w), BF16),
            pltpu.VMEM((n_heads // 2, head_dim, 2 * n_tok), F32),
            pltpu.VMEM((n_heads // 2, 8, 2 * n_tok), F32),
            pltpu.VMEM((n_heads // 2, 8, 2 * n_tok), F32),
            pltpu.VMEM((2, n_tok, half_w), BF16),
            pltpu.VMEM((n_tok, half_w), BF16),
            pltpu.VMEM((n_tok, d_model), F32),
            pltpu.SemaphoreType.DMA((4,)),
            pltpu.SemaphoreType.DMA((2,)),
            pltpu.SemaphoreType.DMA((n_layers, n_copy)),
            pltpu.SemaphoreType.DMA((n_layers, n_copy)),
            pltpu.SemaphoreType.DMA((n_heads // 2 * 4,)),
            pltpu.SemaphoreType.DMA((n_heads + 4,)),
            pltpu.SemaphoreType.DMA((2 * n_heads + 4,)),
            pltpu.SemaphoreType.DMA((n_heads,)),
            pltpu.SemaphoreType.DMA((n_cp // 2,)),
            pltpu.SemaphoreType.DMA((n_cp // 2,)),
            pltpu.SemaphoreType.DMA((n_cp // 2,)),
            pltpu.SemaphoreType.DMA((n_cp // 2,)),
            pltpu.SemaphoreType.DMA((n_heads,)),
            pltpu.SemaphoreType.DMA((n_heads,)),
        ]
        return pl.pallas_call(
            functools.partial(kernel, n_cp, n_layers, n_heads, head_dim),
            out_shape=jax.ShapeDtypeStruct(hidden.shape, hidden.dtype),
            in_specs=[hbm, hbm, hbm, hbm, hbm],
            out_specs=vmem,
            scratch_shapes=scratch,
            compiler_params=pltpu.CompilerParams(collective_id=0, has_side_effects=True, vmem_limit_bytes=66_500_000),
        )(hidden, flat_view(w_query), flat_view(w_key), flat_view(w_value),
          w_out.reshape(n_layers, n_heads * head_dim, d_model))

    row_spec = P(("dp", "cp"), None)
    return jax.shard_map(device_body, mesh=mesh, in_specs=(row_spec, P(), P(), P(), P()), out_specs=row_spec, check_vma=False)
```
